128 devices in a mesh: group: 4 (over y), inner: 32 (over z, x, core).
Axes of the slice: x: 4, y: 4, z: 4, core: 2. Of those that a mesh axis runs over, the one named last changes fastest.
Arguments:
- tokens_fwd: bfloat16 [8192, 2048], P(('group', 'inner')), may hold values from -6 to 6
- experts_fwd: int32 [8192, 8], P(('group', 'inner')), may hold values from 0 to 127, all different within a row; in each aligned block of 64 rows (0 to 63, 64 to 127, ...) at most 6 rows name the same one
- scores_fwd: float32 [8192, 8], P(('group', 'inner')), may hold values from 0.05 to 1
- tokens_bwd: bfloat16 [8192, 2048], P(('group', 'inner')), may hold values from -6 to 6
- experts_bwd: int32 [8192, 8], P(('group', 'inner')), may hold values from 0 to 127, all different within a row; in each aligned block of 64 rows (0 to 63, 64 to 127, ...) at most 6 rows name the same one
- scores_bwd: float32 [8192, 8], P(('group', 'inner')), may hold values from 0.05 to 1
- cotangent: bfloat16 [8192, 2048], P(('group', 'inner')), may hold values from -6 to 6
- w_in: bfloat16 [128, 2048, 1536], P(('group', 'inner')), may hold values from -0.125 to 0.125
- w_down: bfloat16 [128, 768, 2048], P(('group', 'inner')), may hold values from -0.21875 to 0.21875
Outputs:
- output_fwd: bfloat16 [8192, 2048], P(('group', 'inner'))
- grad_tokens: bfloat16 [8192, 2048], P(('group', 'inner'))
- grad_w_in: bfloat16 [128, 2048, 1536], P(('group', 'inner'))
- grad_w_down: bfloat16 [128, 768, 2048], P(('group', 'inner'))
The draws below stay inside these ranges and needn't reach their ends.
Inputs may be any that keep to these rules, and one draw needn't show every extreme that they name: `experts_fwd`: each token names 8 different experts; among the tokens of one device at most 6 name any one expert. `experts_bwd`: each token names 8 different experts; among the tokens of one device at most 6 name any one expert.
All inputs are finite; a program needn't handle non-finite values.
Results may differ from the reference program's by a relative error of at most 0.0064.
Values may be sent and summed in bfloat16 or wider, within the bound.
No kernel may reach another device: no remote copies, remote signals or barrier semaphores. Data moves between devices by JAX's collectives and lax.ppermute only.
A program may use at most 128 MiB of HBM per device.

```python
import math
import jax
import jax.numpy as jnp
import numpy as np
from jax import lax

D = 2048
FF = 768
TOP = 8
TOK_DEV = 64
EXPERTS = 128
CAP = 6
TOKENS = 8192


def levels(stream_key, dims, cuts, low, top_value):
    factor_of = 1.0
    for dim, parts in cuts:
        heights = jax.random.uniform(jax.random.fold_in(jax.random.fold_in(stream_key, 6), dim), (parts,), jnp.float32, low / len(cuts), top_value / len(cuts))
        factor_of = factor_of * jnp.repeat(jnp.exp(heights), dims[dim] // parts).reshape((-1,) + (1,) * (len(dims) - 1 - dim))
    return factor_of


def shared_out(own_key, own, number, rows, count, top, reach, lean):
    ranking = jax.random.permutation(own_key, count)
    crowded, ordinary = load_shares(count, rows * top, reach, lean, True), load_shares(count, rows * top, reach, lean, False)
    places = jnp.arange(count)

    def named(sizes, turn):
        used = int((sizes > 0).sum())
        fixed = max(1, used // 4)
        moved = fixed + (places - fixed + turn * (used - fixed)) % max(1, count - fixed)
        return jnp.zeros((count,), jnp.int32).at[ranking[jnp.where(places < fixed, places, moved)]].set(jnp.asarray(sizes, jnp.int32))

    sizes = jnp.where(number % 4 == 0, named(crowded, number // 4), named(ordinary, number - number // 4 - 1))
    mixed = jax.random.permutation(jax.random.fold_in(own, 3), count)
    donor, receiver = mixed[0:count // 2 * 2:2], mixed[1:count // 2 * 2:2]
    room = jnp.minimum(sizes[donor] - 1, reach - sizes[receiver]) // 2
    room = jnp.where((donor == ranking[0]) | (receiver == ranking[0]) | (sizes[receiver] == 0), 0, jnp.maximum(room, 0))
    moved = jax.random.randint(jax.random.fold_in(own, 4), (count // 2,), 0, 1 << 20) % (room + 1)
    sizes = sizes.at[donor].add(-moved).at[receiver].add(moved)
    members = jnp.searchsorted(jnp.cumsum(sizes), jnp.arange(rows * top), side="right").astype(jnp.int32)
    table = members.reshape(top, rows).T
    table = table[jax.random.permutation(jax.random.fold_in(own, 1), rows)]
    turn = jax.random.randint(jax.random.fold_in(own, 2), (rows, 1), 0, top)
    return jnp.take_along_axis(table, (jnp.arange(top)[None, :] + turn) % top, axis=1)


def load_shares(amount, total, reach, slope, full):
    loads = [(1 << 20) // math.isqrt(grade ** slope) + 1 for grade in range(1, amount + 1)]
    largest = reach if full else min(reach, max(-(-total // amount), total * loads[0] // sum(loads)))
    least = 1 if total - largest >= amount - 1 else 0
    given, rest = [largest] + [least] * (amount - 1), total - largest - least * (amount - 1)
    while rest > 0:
        free = [i for i in range(1, amount) if given[i] < largest] or [i for i in range(1, amount) if given[i] < reach]
        whole, budget = sum([loads[i] for i in free]), rest
        for i in free:
            addition = min(reach - given[i], max(1, budget * loads[i] // whole), rest)
            given[i] = given[i] + addition
            rest = rest - addition
    return np.array(given)


def scatter_about(stream_key, shape, deviation, limit, shards=(), held_as=jnp.bfloat16):
    result = deviation * jax.random.normal(stream_key, shape, jnp.float32)
    if shards:
        result = result * levels(stream_key, shape, shards, -0.22, 0.18)
    return jnp.clip(result, -limit, limit).astype(held_as)


def setup_inputs(seed: int = 0) -> dict:
    seeds = jax.random.split(jax.random.key(seed), 10)
    tokens_fwd = scatter_about(seeds[0], (TOKENS, D), 1.0, 6.0, ((0, 128),))
    experts_fwd_keys = jax.random.split(jax.random.fold_in(seeds[1], 1), TOKENS // TOK_DEV)
    experts_fwd_turns = jax.random.permutation(jax.random.fold_in(seeds[1], 3), TOKENS // TOK_DEV)
    experts_fwd = jax.vmap(lambda own, number: shared_out(jax.random.fold_in(seeds[1], 2), own, number, TOK_DEV, EXPERTS, TOP, CAP, 2))(experts_fwd_keys, experts_fwd_turns).reshape((TOKENS, TOP))
    scores_fwd = jnp.clip(jnp.exp(math.log(1.0) - 2.9957323 * jax.random.uniform(seeds[2], (TOKENS, TOP), jnp.float32) ** levels(seeds[2], (TOKENS, TOP), ((0, 128),), -0.2, 0.2)), 0.05, 1.0)
    tokens_bwd = scatter_about(seeds[3], (TOKENS, D), 1.0, 6.0, ((0, 128),))
    experts_bwd_keys = jax.random.split(jax.random.fold_in(seeds[4], 1), TOKENS // TOK_DEV)
    experts_bwd_turns = jax.random.permutation(jax.random.fold_in(seeds[4], 3), TOKENS // TOK_DEV)
    experts_bwd = jax.vmap(lambda own, number: shared_out(jax.random.fold_in(seeds[4], 2), own, number, TOK_DEV, EXPERTS, TOP, CAP, 2))(experts_bwd_keys, experts_bwd_turns).reshape((TOKENS, TOP))
    scores_bwd = jnp.clip(jnp.exp(math.log(1.0) - 2.9957323 * jax.random.uniform(seeds[5], (TOKENS, TOP), jnp.float32) ** levels(seeds[5], (TOKENS, TOP), ((0, 128),), -0.2, 0.2)), 0.05, 1.0)
    cotangent = scatter_about(seeds[6], (TOKENS, D), 1.0, 6.0, ((0, 128),))
    w_in = scatter_about(seeds[7], (EXPERTS, D, 2 * FF), D ** -0.5, 0.125, ((0, 128),))
    w_down = scatter_about(seeds[8], (EXPERTS, FF, D), FF ** -0.5, 0.21875, ((0, 128),))
    return {"tokens_fwd": tokens_fwd, "experts_fwd": experts_fwd, "scores_fwd": scores_fwd, "tokens_bwd": tokens_bwd, "experts_bwd": experts_bwd, "scores_bwd": scores_bwd, "cotangent": cotangent, "w_in": w_in, "w_down": w_down}


def expert_forward(tok_rows, w_in_e, w_down_e):
    width = w_down_e.shape[0]
    projected = jnp.dot(tok_rows, w_in_e, preferred_element_type=jnp.float32)
    gate_part = projected[:, :width]
    up_part = projected[:, width:]
    hidden = (gate_part * jax.nn.sigmoid(gate_part) * up_part).astype(jnp.bfloat16)
    return jnp.dot(hidden, w_down_e, preferred_element_type=jnp.float32).astype(jnp.bfloat16)


def expert_backward(tok_rows, cot_rows, w_in_e, w_down_e):
    width = w_down_e.shape[0]
    projected = jnp.dot(tok_rows, w_in_e, preferred_element_type=jnp.float32)
    gate_part = projected[:, :width]
    up_part = projected[:, width:]
    sigmoid_gate = jax.nn.sigmoid(gate_part)
    hidden = (gate_part * sigmoid_gate * up_part).astype(jnp.bfloat16)
    contract_rows = (((0,), (0,)), ((), ()))
    contract_cols = (((1,), (1,)), ((), ()))
    grad_down = lax.dot_general(hidden, cot_rows, contract_rows, preferred_element_type=jnp.float32).astype(jnp.bfloat16)
    d_hidden = lax.dot_general(cot_rows, w_down_e, contract_cols, preferred_element_type=jnp.float32)
    d_gate = d_hidden * up_part * sigmoid_gate * (1.0 + gate_part * (1.0 - sigmoid_gate))
    d_up = d_hidden * gate_part * sigmoid_gate
    d_proj = jnp.concatenate([d_gate, d_up], axis=1).astype(jnp.bfloat16)
    grad_inner = lax.dot_general(tok_rows, d_proj, contract_rows, preferred_element_type=jnp.float32).astype(jnp.bfloat16)
    row_grad = lax.dot_general(d_proj, w_in_e, contract_cols, preferred_element_type=jnp.float32).astype(jnp.bfloat16)
    return row_grad, grad_inner, grad_down


def assignment_tables(expert_ids, scores):
    blocks = TOKENS // TOK_DEV
    flat_ids = expert_ids.reshape(blocks, TOK_DEV * TOP).astype(jnp.int32)
    labels = jnp.arange(EXPERTS, dtype=jnp.int32)
    onehot = (flat_ids[:, :, None] == labels[None, None, :]).astype(jnp.int32)
    before = jnp.cumsum(onehot, axis=1) - onehot
    slot_pos = jnp.sum(before * onehot, axis=2).astype(jnp.int32)
    block_of = jnp.arange(blocks, dtype=jnp.int32)[:, None]
    token_of = block_of * TOK_DEV + jnp.arange(TOK_DEV * TOP, dtype=jnp.int32)[None, :] // TOP
    target = ((flat_ids * blocks + block_of) * CAP + slot_pos).reshape(-1).astype(jnp.int32)
    source = jnp.full((EXPERTS * blocks * CAP,), TOKENS, jnp.int32).at[target].set(token_of.reshape(-1).astype(jnp.int32))
    weights = scores / jnp.sum(scores, axis=1, keepdims=True)
    scaled = jnp.zeros((EXPERTS * blocks * CAP,), jnp.float32).at[target].set(weights.reshape(-1).astype(jnp.float32))
    return source.reshape(EXPERTS, blocks * CAP), scaled.reshape(EXPERTS, blocks * CAP)


def reference(tokens_fwd, experts_fwd, scores_fwd, tokens_bwd, experts_bwd, scores_bwd, cotangent, w_in, w_down):
    source_fwd, scaled_fwd = assignment_tables(experts_fwd, scores_fwd)
    source_bwd, scaled_bwd = assignment_tables(experts_bwd, scores_bwd)
    zero_row = jnp.zeros((1, D), jnp.bfloat16)
    fwd_padded = jnp.concatenate([tokens_fwd, zero_row], axis=0)
    bwd_padded = jnp.concatenate([tokens_bwd, zero_row], axis=0)
    cot_padded = jnp.concatenate([cotangent, zero_row], axis=0)

    def expert_step(totals, inputs):
        out_total, grad_total = totals
        w_in_e, w_down_e, src_f, scl_f, src_b, scl_b = inputs
        expert_out = expert_forward(fwd_padded[src_f], w_in_e, w_down_e)
        out_total = out_total.at[src_f].add(scl_f[:, None] * expert_out.astype(jnp.float32))
        cot_rows = (scl_b[:, None] * cot_padded[src_b].astype(jnp.float32)).astype(jnp.bfloat16)
        row_grad, grad_inner, grad_down = expert_backward(bwd_padded[src_b], cot_rows, w_in_e, w_down_e)
        grad_total = grad_total.at[src_b].add(row_grad.astype(jnp.float32))
        return (out_total, grad_total), (grad_inner, grad_down)

    start = (jnp.zeros((TOKENS + 1, D), jnp.float32), jnp.zeros((TOKENS + 1, D), jnp.float32))
    (out_total, grad_total), (grad_w_in, grad_w_down) = lax.scan(
        expert_step, start, (w_in, w_down, source_fwd, scaled_fwd, source_bwd, scaled_bwd))
    output_fwd = out_total[:TOKENS].astype(jnp.bfloat16)
    grad_tokens = grad_total[:TOKENS].astype(jnp.bfloat16)
    return output_fwd, grad_tokens, grad_w_in, grad_w_down
```

```python
import functools

import jax
import jax.numpy as jnp
import numpy as np
from jax import lax
from jax.experimental import pallas as pl
from jax.experimental.pallas import tpu as pltpu
from jax.sharding import PartitionSpec as P

AXES = ("group", "inner")
PARTS = 4
GROUP = 8
F32 = jnp.float32
BF16 = jnp.bfloat16
ROWS_BY_ROWS = (((0,), (0,)), ((), ()))
COLS_BY_COLS = (((1,), (1,)), ((), ()))


def call(body, grid, in_specs, out_specs, out_shape, cost, scratch=()):
    return pl.pallas_call(
        body,
        grid=grid,
        in_specs=in_specs,
        out_specs=out_specs,
        out_shape=out_shape,
        scratch_shapes=list(scratch),
        compiler_params=pltpu.CompilerParams(
            dimension_semantics=("arbitrary",) * len(grid)
        ),
        cost_estimate=pl.CostEstimate(
            flops=cost[0], bytes_accessed=cost[1], transcendentals=0
        ),
    )


def whole(shape):
    return pl.BlockSpec(shape, lambda i: (0,) * len(shape))


def slots_body(experts, chunk, capacity, ids_f, sc_f, ids_b, sc_b, key_f, wgt_f, key_b, wgt_b):
    tok, top = ids_f.shape
    wide = PARTS * tok
    lane = lax.broadcasted_iota(jnp.int32, (tok, wide), 1)
    row = lax.broadcasted_iota(jnp.int32, (tok, wide), 0)
    spread = jnp.where(lane % tok == row, 1.0, 0.0)
    earlier = jnp.where(row < lane % tok, 1.0, 0.0).astype(BF16)
    label = lax.broadcasted_iota(jnp.int32, (experts, wide), 0)
    part = lax.broadcasted_iota(jnp.int32, (1, wide), 1) // tok
    for ids, sc, key, wgt in ((ids_f, sc_f, key_f, wgt_f), (ids_b, sc_b, key_b, wgt_b)):
        named = lax.dot_general(
            ids[...].astype(F32).astype(BF16), spread.astype(BF16), ROWS_BY_ROWS,
            preferred_element_type=F32,
        ).astype(jnp.int32)
        hits = [label == named[j : j + 1, :] for j in range(top)]
        chosen = jnp.zeros((experts, wide), F32)
        for hit in hits:
            chosen = chosen + jnp.where(hit, 1.0, 0.0)
        before = jnp.dot(
            chosen[:, :tok].astype(BF16), earlier, preferred_element_type=F32
        )
        for j in range(top):
            slot = jnp.sum(jnp.where(hits[j], before, 0.0), axis=0, keepdims=True)
            key[j : j + 1, :] = (
                named[j : j + 1, :] * chunk + part * capacity + slot.astype(jnp.int32)
            )
        share = lax.dot_general(
            sc[...], spread, ROWS_BY_ROWS,
            preferred_element_type=F32, precision=lax.Precision.HIGHEST,
        )
        wgt[...] = share / jnp.sum(share, axis=0, keepdims=True)


def slots(experts, capacity, ids_f, sc_f, ids_b, sc_b):
    tok, top = ids_f.shape
    small = (top, PARTS * tok)
    return call(
        functools.partial(slots_body, experts, PARTS * capacity, capacity),
        (1,),
        [whole((tok, top))] * 4,
        [whole(small)] * 4,
        [
            jax.ShapeDtypeStruct(small, jnp.int32),
            jax.ShapeDtypeStruct(small, F32),
        ]
        * 2,
        (10_000_000, 100_000),
    )(ids_f, sc_f, ids_b, sc_b)


def stacked(ref):
    step = ref.shape[1] // PARTS
    return jnp.concatenate([ref[:, q * step : (q + 1) * step] for q in range(PARTS)], axis=0)


def send_body(rows, weighted, key, wgt, *refs):
    *tables, out = refs
    top, wide = key.shape
    step = tables[0].shape[1] // PARTS
    mine = pl.program_id(0) * rows + lax.broadcasted_iota(jnp.int32, (rows, wide), 0)
    pick = jnp.zeros((rows, wide), F32)
    load = jnp.zeros((rows, wide), F32)
    for j in range(top):
        hit = mine == key[j : j + 1, :]
        pick = jnp.where(hit, 1.0, pick)
        if any(weighted):
            load = jnp.where(hit, wgt[j : j + 1, :], load)
    pick = pick.astype(BF16)
    scale = jnp.sum(load, axis=1, keepdims=True) if any(weighted) else None
    for i, table in enumerate(tables):
        got = jnp.dot(pick, stacked(table), preferred_element_type=F32)
        if weighted[i]:
            got = got * scale
        out[:, i * step : (i + 1) * step] = got.astype(BF16)


def send(total, key, wgt, tables, weighted):
    tok, width = tables[0].shape
    top, wide = key.shape
    n = len(tables)
    rows = total // 8
    return call(
        functools.partial(send_body, rows, weighted),
        (8,),
        [whole((top, wide))] * 2 + [whole((tok, width))] * n,
        pl.BlockSpec((rows, n * width // PARTS), lambda i: (i, 0)),
        jax.ShapeDtypeStruct((total, n * width // PARTS), BF16),
        (2 * total * wide * n * width // PARTS, 2 * total * n * width // PARTS),
    )(key, wgt, *tables)


def order(capacity):
    size = GROUP * PARTS * capacity
    matrix = np.zeros((size, size), np.float32)
    for s in range(GROUP):
        for q in range(PARTS):
            for c in range(capacity):
                matrix[(q * GROUP + s) * capacity + c, (s * PARTS + q) * capacity + c] = 1.0
    return matrix


def unpack_body(n, perm, got, *outs):
    step = got.shape[1] // n
    count = outs[0].shape[0]
    rows = jnp.dot(perm[...], got[...], preferred_element_type=F32).astype(BF16)
    for i, out in enumerate(outs):
        for q in range(PARTS):
            out[:, q * step : (q + 1) * step] = rows[
                q * count : (q + 1) * count, i * step : (i + 1) * step
            ]


def unpack(perm, got, n):
    size = perm.shape[0]
    total, wide = got.shape
    count = size // PARTS
    step = wide // n
    shape = (total // PARTS, PARTS * step)
    return call(
        functools.partial(unpack_body, n),
        (total // size,),
        [whole((size, size)), pl.BlockSpec((size, wide), lambda i: (i, 0))],
        [pl.BlockSpec((count, PARTS * step), lambda i: (i, 0))] * n,
        [jax.ShapeDtypeStruct(shape, BF16)] * n,
        (2 * total * size * wide, 4 * total * wide),
    )(perm, got)


def pack_body(perm, rows, out):
    out[...] = lax.dot_general(
        perm[...], stacked(rows), ROWS_BY_ROWS, preferred_element_type=F32
    ).astype(BF16)


def pack(perm, rows):
    size = perm.shape[0]
    total, width = rows.shape
    count = size // PARTS
    return call(
        pack_body,
        (total // count,),
        [whole((size, size)), pl.BlockSpec((count, width), lambda i: (i, 0))],
        pl.BlockSpec((size, width // PARTS), lambda i: (i, 0)),
        jax.ShapeDtypeStruct((total * PARTS, width // PARTS), BF16),
        (2 * total * size * width, 4 * total * width),
    )(perm, rows)


def combine_body(rows, weighted, key, wgt, got, out, total):
    top, wide = key.shape
    step = pl.program_id(0)
    mine = step * rows + lax.broadcasted_iota(jnp.int32, (rows, wide), 0)
    load = jnp.zeros((rows, wide), F32)
    for j in range(top):
        load = jnp.where(mine == key[j : j + 1, :], wgt[j : j + 1, :] if weighted else 1.0, load)
    high = load.astype(BF16)
    part = lax.dot_general(high, got[...], ROWS_BY_ROWS, preferred_element_type=F32)
    if weighted:
        low = (load - high.astype(F32)).astype(BF16)
        part = part + lax.dot_general(low, got[...], ROWS_BY_ROWS, preferred_element_type=F32)

    @pl.when(step == 0)
    def _():
        total[...] = part

    @pl.when(step > 0)
    def _():
        total[...] += part

    @pl.when(step == pl.num_programs(0) - 1)
    def _():
        tok, width = out.shape
        piece = width // PARTS
        for q in range(PARTS):
            out[:, q * piece : (q + 1) * piece] = total[q * tok : (q + 1) * tok, :].astype(BF16)


def combine(key, wgt, got, weighted):
    top, wide = key.shape
    count, piece = got.shape
    rows = count // 8
    tok = wide // PARTS
    return call(
        functools.partial(combine_body, rows, weighted),
        (8,),
        [whole((top, wide))] * 2 + [pl.BlockSpec((rows, piece), lambda i: (i, 0))],
        whole((tok, piece * PARTS)),
        jax.ShapeDtypeStruct((tok, piece * PARTS), BF16),
        (4 * count * wide * piece, 2 * count * piece),
        [pltpu.VMEM((wide, piece), F32)],
    )(key, wgt, got)


def exchange(x):
    return lax.all_to_all(x, AXES, split_axis=0, concat_axis=0, tiled=True)


def expert_forward(x, w_in, w_down):
    width = w_down.shape[0]
    projected = jnp.dot(x, w_in, preferred_element_type=F32)
    g, u = projected[:, :width], projected[:, width:]
    hidden = (g * jax.nn.sigmoid(g) * u).astype(BF16)
    return jnp.dot(hidden, w_down, preferred_element_type=F32).astype(BF16)


def expert_backward(x, cot, w_in, w_down):
    width = w_down.shape[0]
    projected = jnp.dot(x, w_in, preferred_element_type=F32)
    g, u = projected[:, :width], projected[:, width:]
    s = jax.nn.sigmoid(g)
    hidden = (g * s * u).astype(BF16)
    d_hidden = lax.dot_general(cot, w_down, COLS_BY_COLS, preferred_element_type=F32)
    d_gate = d_hidden * u * s * (1.0 + g * (1.0 - s))
    d_up = d_hidden * g * s
    d_proj = jnp.concatenate([d_gate, d_up], axis=1).astype(BF16)
    row_grad = lax.dot_general(
        d_proj, w_in, COLS_BY_COLS, preferred_element_type=F32
    ).astype(BF16)
    return row_grad, hidden, d_proj


def shards(
    tokens_fwd, experts_fwd, scores_fwd, tokens_bwd, experts_bwd, scores_bwd, cotangent, w_in, w_down
):
    devices = lax.axis_size("group") * lax.axis_size("inner")
    tok, top = experts_fwd.shape
    capacity = max(2, 3 * tok * top // (2 * devices))
    total = devices * capacity * PARTS
    perm = jnp.asarray(order(capacity), BF16)
    w_in, w_down = w_in[0], w_down[0]

    key_f, wgt_f, key_b, wgt_b = slots(
        devices, capacity, experts_fwd, scores_fwd, experts_bwd, scores_bwd
    )
    out_b = send(total, key_b, wgt_b, (tokens_bwd, cotangent), (False, True))
    in_b = exchange(out_b)
    out_f = send(total, key_f, wgt_f, (tokens_fwd,), (False,))
    out_f, in_b = lax.optimization_barrier((out_f, in_b))
    in_f = exchange(out_f)

    rows_b, cot_b = unpack(perm, in_b, 2)
    row_grad, hidden, d_proj = expert_backward(rows_b, cot_b, w_in, w_down)
    back_b = pack(perm, row_grad)
    back_b, in_f = lax.optimization_barrier((back_b, in_f))
    home_b = exchange(back_b)

    (rows_f,) = unpack(perm, in_f, 1)
    back_f = pack(perm, expert_forward(rows_f, w_in, w_down))
    grad_down = lax.dot_general(
        hidden, cot_b, ROWS_BY_ROWS, preferred_element_type=F32
    ).astype(BF16)
    grad_in = lax.dot_general(
        rows_b, d_proj, ROWS_BY_ROWS, preferred_element_type=F32
    ).astype(BF16)
    back_f, home_b = lax.optimization_barrier((back_f, home_b))
    home_f = exchange(back_f)

    grad_tokens = combine(key_b, wgt_b, home_b, False)
    output_fwd = combine(key_f, wgt_f, home_f, True)
    return output_fwd, grad_tokens, grad_in[None], grad_down[None]


def solution(mesh):
    rows = P(AXES, None)
    cube = P(AXES, None, None)
    return jax.shard_map(
        shards,
        mesh=mesh,
        in_specs=(rows,) * 7 + (cube,) * 2,
        out_specs=(rows, rows, cube, cube),
        check_vma=False,
    )
```

```python
import functools

import jax
import jax.numpy as jnp
from jax import lax
from jax.experimental import pallas as pl
from jax.experimental.pallas import tpu as pltpu
from jax.sharding import PartitionSpec as P


AXES = ("group", "inner")
PARTS = 4
LANES = 128
F32 = jnp.float32
BF16 = jnp.bfloat16
ROWS_BY_ROWS = (((0,), (0,)), ((), ()))
COLS_BY_COLS = (((1,), (1,)), ((), ()))


def call(body, grid, in_specs, out_specs, out_shape, cost, scratch=()):
    return pl.pallas_call(
        body,
        grid=grid,
        in_specs=in_specs,
        out_specs=out_specs,
        out_shape=out_shape,
        scratch_shapes=list(scratch),
        compiler_params=pltpu.CompilerParams(
            dimension_semantics=("arbitrary",) * len(grid)
        ),
        cost_estimate=pl.CostEstimate(
            flops=cost[0], bytes_accessed=cost[1], transcendentals=0
        ),
    )


def whole(shape):
    return pl.BlockSpec(shape, lambda i: (0,) * len(shape))


def spread(pieces, q, rows):
    count, piece = rows.shape
    for k in range(piece // LANES):
        pieces[k, pl.ds(q, count, stride=PARTS), :] = rows[:, k * LANES : (k + 1) * LANES]


def collected(pieces, q, first, piece):
    count = pieces.shape[1] // PARTS
    return jnp.concatenate(
        [
            pieces[k, pl.ds(q, count, stride=PARTS), :]
            for k in range(first // LANES, (first + piece) // LANES)
        ],
        axis=1,
    ).astype(BF16)


def fill(pieces, chunks):
    for k in range(pieces.shape[0]):
        pieces[k] = chunks[:, k * LANES : (k + 1) * LANES].astype(F32)


def flush(pieces, out, first):
    for k in range(pieces.shape[0]):
        out[:, first + k * LANES : first + (k + 1) * LANES] = pieces[k].astype(BF16)


def place(experts, capacity, ids, sc, key, wgt):
    top, tok = ids.shape
    label = lax.broadcasted_iota(jnp.int32, (experts, tok), 0)
    hits = [label == ids[j : j + 1, :] for j in range(top)]
    chosen = jnp.zeros((experts, tok), F32)
    for hit in hits:
        chosen = jnp.where(hit, 1.0, chosen)
    earlier = lax.broadcasted_iota(jnp.int32, (tok, tok), 0) < lax.broadcasted_iota(
        jnp.int32, (tok, tok), 1
    )
    before = jnp.dot(
        chosen.astype(BF16),
        jnp.where(earlier, 1.0, 0.0).astype(BF16),
        preferred_element_type=F32,
    )
    for j in range(top):
        slot = jnp.sum(jnp.where(hits[j], before, 0.0), axis=0, keepdims=True)
        key[j : j + 1, :] = ids[j : j + 1, :] * capacity + slot.astype(jnp.int32)
    share = sc[...]
    wgt[...] = share / jnp.sum(share, axis=0, keepdims=True)


def send_body(experts, capacity, weighted, ids, sc, *refs):
    *tables, out, key, wgt, pieces = refs
    top, tok = ids.shape
    rows = out.shape[0] // PARTS
    piece = tables[0].shape[1] // PARTS

    @pl.when(pl.program_id(0) == 0)
    def _():
        place(experts, capacity, ids, sc, key, wgt)

    mine = pl.program_id(0) * rows + lax.broadcasted_iota(jnp.int32, (rows, tok), 0)
    pick = jnp.zeros((rows, tok), F32)
    load = jnp.zeros((rows, tok), F32)
    for j in range(top):
        hit = mine == key[j : j + 1, :]
        pick = jnp.where(hit, 1.0, pick)
        load = jnp.where(hit, wgt[j : j + 1, :], load)
    pick = pick.astype(BF16)
    scale = jnp.sum(load, axis=1, keepdims=True)
    for i, table in enumerate(tables):
        for q in range(PARTS):
            got = jnp.dot(
                pick, table[:, q * piece : (q + 1) * piece], preferred_element_type=F32
            )
            if weighted[i]:
                got = got * scale
            spread(pieces, q, got)
        flush(pieces, out, i * piece)


def send(experts, capacity, ids, sc, tables, weighted):
    tok, width = tables[0].shape
    n = len(tables)
    total = experts * capacity * PARTS
    piece = width // PARTS
    steps = 8
    return call(
        functools.partial(send_body, experts, capacity, weighted),
        (steps,),
        [whole(ids.shape)] * 2 + [whole((tok, width))] * n,
        [
            pl.BlockSpec((total // steps, n * piece), lambda i: (i, 0)),
            whole(ids.shape),
            whole(ids.shape),
        ],
        [
            jax.ShapeDtypeStruct((total, n * piece), BF16),
            jax.ShapeDtypeStruct(ids.shape, jnp.int32),
            jax.ShapeDtypeStruct(ids.shape, F32),
        ],
        (2 * total * tok * n * piece, 2 * total * n * piece),
        [pltpu.VMEM((piece // LANES, total // steps, LANES), F32)],
    )(ids, sc, *tables)


def unpack_body(n, got, *refs):
    *outs, pieces = refs
    piece = got.shape[1] // n
    fill(pieces, got)
    for i, out in enumerate(outs):
        for q in range(PARTS):
            out[:, q * piece : (q + 1) * piece] = collected(pieces, q, i * piece, piece)


def unpack(got, n):
    total, wide = got.shape
    steps = 8
    width = PARTS * wide // n
    return call(
        functools.partial(unpack_body, n),
        (steps,),
        [pl.BlockSpec((total // steps, wide), lambda i: (i, 0))],
        [pl.BlockSpec((total // PARTS // steps, width), lambda i: (i, 0))] * n,
        [jax.ShapeDtypeStruct((total // PARTS, width), BF16)] * n,
        (400 * total * wide, 4 * total * wide),
        [pltpu.VMEM((wide // LANES, total // steps, LANES), F32)],
    )(got)


def pack_body(rows, out, pieces):
    width = rows.shape[1]
    piece = width // PARTS
    for q in range(PARTS):
        spread(pieces, q, rows[:, q * piece : (q + 1) * piece].astype(F32))
    flush(pieces, out, 0)


def pack(rows):
    total, width = rows.shape
    steps = 8
    piece = width // PARTS
    count = total // steps
    return call(
        pack_body,
        (steps,),
        [pl.BlockSpec((count, width), lambda i: (i, 0))],
        pl.BlockSpec((count * PARTS, piece), lambda i: (i, 0)),
        jax.ShapeDtypeStruct((total * PARTS, piece), BF16),
        (400 * total * width, 4 * total * width),
        [pltpu.VMEM((piece // LANES, count * PARTS, LANES), F32)],
    )(rows)


def combine_body(weighted, key, wgt, got, out, total, pieces):
    top, tok = key.shape
    step = pl.program_id(0)
    rows = got.shape[0] // PARTS
    piece = got.shape[1]
    mine = step * rows + lax.broadcasted_iota(jnp.int32, (rows, tok), 0)
    load = jnp.zeros((rows, tok), F32)
    for j in range(top):
        load = jnp.where(mine == key[j : j + 1, :], wgt[j : j + 1, :] if weighted else 1.0, load)
    high = load.astype(BF16)
    low = (load - high.astype(F32)).astype(BF16)
    fill(pieces, got)

    @pl.when(step == 0)
    def _():
        total[...] = jnp.zeros_like(total)

    for q in range(PARTS):
        lanes = slice(q * piece, (q + 1) * piece)
        part = collected(pieces, q, 0, piece)
        more = lax.dot_general(high, part, ROWS_BY_ROWS, preferred_element_type=F32)
        if weighted:
            more = more + lax.dot_general(low, part, ROWS_BY_ROWS, preferred_element_type=F32)
        total[:, lanes] += more

    @pl.when(step == pl.num_programs(0) - 1)
    def _():
        out[...] = total[...].astype(BF16)


def combine(key, wgt, got, weighted):
    top, tok = key.shape
    count, piece = got.shape
    steps = 4
    rows = count // steps
    return call(
        functools.partial(combine_body, weighted),
        (steps,),
        [whole((top, tok))] * 2 + [pl.BlockSpec((rows, piece), lambda i: (i, 0))],
        whole((tok, piece * PARTS)),
        jax.ShapeDtypeStruct((tok, piece * PARTS), BF16),
        (4 * count * tok * piece, 2 * count * piece),
        [pltpu.VMEM((tok, piece * PARTS), F32), pltpu.VMEM((piece // LANES, rows, LANES), F32)],
    )(key, wgt, got)


def exchange(x):
    return lax.all_to_all(x, AXES, split_axis=0, concat_axis=0, tiled=True)


def expert_forward(x, w_in, w_down):
    width = w_down.shape[0]
    projected = jnp.dot(x, w_in, preferred_element_type=F32)
    g, u = projected[:, :width], projected[:, width:]
    hidden = (g * jax.nn.sigmoid(g) * u).astype(BF16)
    return jnp.dot(hidden, w_down, preferred_element_type=F32).astype(BF16)


def expert_backward(x, cot, w_in, w_down):
    width = w_down.shape[0]
    projected = jnp.dot(x, w_in, preferred_element_type=F32)
    g, u = projected[:, :width], projected[:, width:]
    s = jax.nn.sigmoid(g)
    hidden = (g * s * u).astype(BF16)
    d_hidden = lax.dot_general(cot, w_down, COLS_BY_COLS, preferred_element_type=F32)
    d_gate = d_hidden * u * s * (1.0 + g * (1.0 - s))
    d_up = d_hidden * g * s
    d_proj = jnp.concatenate([d_gate, d_up], axis=1).astype(BF16)
    row_grad = lax.dot_general(
        d_proj, w_in, COLS_BY_COLS, preferred_element_type=F32
    ).astype(BF16)
    return row_grad, hidden, d_proj


def layer(
    tokens_fwd, experts_fwd, scores_fwd, tokens_bwd, experts_bwd, scores_bwd, cotangent, w_in, w_down
):
    devices = lax.axis_size("group") * lax.axis_size("inner")
    tok, top = experts_fwd.shape
    capacity = max(2, 3 * tok * top // (2 * devices))
    w_in, w_down = w_in[0], w_down[0]

    out_b, key_b, wgt_b = send(
        devices, capacity, experts_bwd.T, scores_bwd.T, (tokens_bwd, cotangent), (False, True)
    )
    in_b = exchange(out_b)
    out_f, key_f, wgt_f = send(
        devices, capacity, experts_fwd.T, scores_fwd.T, (tokens_fwd,), (False,)
    )
    out_f, in_b = lax.optimization_barrier((out_f, in_b))
    in_f = exchange(out_f)

    rows_b, cot_b = unpack(in_b, 2)
    row_grad, hidden, d_proj = expert_backward(rows_b, cot_b, w_in, w_down)
    back_b = pack(row_grad)
    back_b, in_f = lax.optimization_barrier((back_b, in_f))
    home_b = exchange(back_b)

    (rows_f,) = unpack(in_f, 1)
    back_f = pack(expert_forward(rows_f, w_in, w_down))
    grad_down = lax.dot_general(
        hidden, cot_b, ROWS_BY_ROWS, preferred_element_type=F32
    ).astype(BF16)
    grad_in = lax.dot_general(
        rows_b, d_proj, ROWS_BY_ROWS, preferred_element_type=F32
    ).astype(BF16)
    back_f, home_b = lax.optimization_barrier((back_f, home_b))
    home_f = exchange(back_f)

    grad_tokens = combine(key_b, wgt_b, home_b, False)
    output_fwd = combine(key_f, wgt_f, home_f, True)
    return output_fwd, grad_tokens, grad_in[None], grad_down[None]


def solution(mesh):
    rows = P(AXES, None)
    cube = P(AXES, None, None)
    return jax.shard_map(
        layer,
        mesh=mesh,
        in_specs=(rows,) * 7 + (cube,) * 2,
        out_specs=(rows, rows, cube, cube),
        check_vma=False,
    )
```

```python
import functools

import jax
import jax.numpy as jnp
from jax import lax
from jax.experimental import pallas as pl
from jax.experimental.pallas import tpu as pltpu
from jax.sharding import PartitionSpec as P


AXES = ("group", "inner")
PARTS = 4
LANES = 128
F32 = jnp.float32
BF16 = jnp.bfloat16
ROWS_BY_ROWS = (((0,), (0,)), ((), ()))
COLS_BY_COLS = (((1,), (1,)), ((), ()))


def call(body, grid, in_specs, out_specs, out_shape, cost, scratch=()):
    return pl.pallas_call(
        body,
        grid=grid,
        in_specs=in_specs,
        out_specs=out_specs,
        out_shape=out_shape,
        scratch_shapes=list(scratch),
        compiler_params=pltpu.CompilerParams(
            dimension_semantics=("arbitrary",) * len(grid)
        ),
        cost_estimate=pl.CostEstimate(
            flops=cost[0], bytes_accessed=cost[1], transcendentals=0
        ),
    )


def whole(shape):
    return pl.BlockSpec(shape, lambda i: (0,) * len(shape))


def spread(pieces, q, rows):
    count, piece = rows.shape
    for k in range(piece // LANES):
        pieces[k, pl.ds(q, count, stride=PARTS), :] = rows[:, k * LANES : (k + 1) * LANES]


def collected(pieces, q, first, piece):
    count = pieces.shape[1] // PARTS
    return jnp.concatenate(
        [
            pieces[k, pl.ds(q, count, stride=PARTS), :]
            for k in range(first // LANES, (first + piece) // LANES)
        ],
        axis=1,
    ).astype(BF16)


def fill(pieces, chunks):
    for k in range(pieces.shape[0]):
        pieces[k] = chunks[:, k * LANES : (k + 1) * LANES].astype(F32)


def flush(pieces, out, first):
    for k in range(pieces.shape[0]):
        out[:, first + k * LANES : first + (k + 1) * LANES] = pieces[k].astype(BF16)


def place(experts, capacity, ids, sc, key, wgt):
    top, tok = ids.shape
    label = lax.broadcasted_iota(jnp.int32, (experts, tok), 0)
    hits = [label == ids[j : j + 1, :] for j in range(top)]
    chosen = jnp.zeros((experts, tok), F32)
    for hit in hits:
        chosen = jnp.where(hit, 1.0, chosen)
    earlier = lax.broadcasted_iota(jnp.int32, (tok, tok), 0) < lax.broadcasted_iota(
        jnp.int32, (tok, tok), 1
    )
    before = jnp.dot(
        chosen.astype(BF16),
        jnp.where(earlier, 1.0, 0.0).astype(BF16),
        preferred_element_type=F32,
    )
    for j in range(top):
        slot = jnp.sum(jnp.where(hits[j], before, 0.0), axis=0, keepdims=True)
        key[j : j + 1, :] = ids[j : j + 1, :] * capacity + slot.astype(jnp.int32)
    share = sc[...]
    wgt[...] = share / jnp.sum(share, axis=0, keepdims=True)


def send_body(experts, capacity, weighted, ids, sc, *refs):
    *tables, out, key, wgt, pieces = refs
    top, tok = ids.shape
    rows = out.shape[0] // PARTS
    piece = tables[0].shape[1] // PARTS

    @pl.when(pl.program_id(0) == 0)
    def _():
        place(experts, capacity, ids, sc, key, wgt)

    mine = pl.program_id(0) * rows + lax.broadcasted_iota(jnp.int32, (rows, tok), 0)
    pick = jnp.zeros((rows, tok), F32)
    load = jnp.zeros((rows, tok), F32)
    for j in range(top):
        hit = mine == key[j : j + 1, :]
        pick = jnp.where(hit, 1.0, pick)
        load = jnp.where(hit, wgt[j : j + 1, :], load)
    pick = pick.astype(BF16)
    scale = jnp.sum(load, axis=1, keepdims=True)
    for i, table in enumerate(tables):
        for q in range(PARTS):
            got = jnp.dot(
                pick, table[:, q * piece : (q + 1) * piece], preferred_element_type=F32
            )
            if weighted[i]:
                got = got * scale
            spread(pieces, q, got)
        flush(pieces, out, i * piece)


def send(experts, capacity, ids, sc, tables, weighted):
    tok, width = tables[0].shape
    n = len(tables)
    total = experts * capacity * PARTS
    piece = width // PARTS
    steps = 2
    return call(
        functools.partial(send_body, experts, capacity, weighted),
        (steps,),
        [whole(ids.shape)] * 2 + [whole((tok, width))] * n,
        [
            pl.BlockSpec((total // steps, n * piece), lambda i: (i, 0)),
            whole(ids.shape),
            whole(ids.shape),
        ],
        [
            jax.ShapeDtypeStruct((total, n * piece), BF16),
            jax.ShapeDtypeStruct(ids.shape, jnp.int32),
            jax.ShapeDtypeStruct(ids.shape, F32),
        ],
        (2 * total * tok * n * piece, 2 * total * n * piece),
        [pltpu.VMEM((piece // LANES, total // steps, LANES), F32)],
    )(ids, sc, *tables)


def unpack_body(n, got, *refs):
    *outs, pieces = refs
    piece = got.shape[1] // n
    fill(pieces, got)
    for i, out in enumerate(outs):
        for q in range(PARTS):
            out[:, q * piece : (q + 1) * piece] = collected(pieces, q, i * piece, piece)


def unpack(got, n):
    total, wide = got.shape
    steps = 2
    width = PARTS * wide // n
    return call(
        functools.partial(unpack_body, n),
        (steps,),
        [pl.BlockSpec((total // steps, wide), lambda i: (i, 0))],
        [pl.BlockSpec((total // PARTS // steps, width), lambda i: (i, 0))] * n,
        [jax.ShapeDtypeStruct((total // PARTS, width), BF16)] * n,
        (400 * total * wide, 4 * total * wide),
        [pltpu.VMEM((wide // LANES, total // steps, LANES), F32)],
    )(got)


def pack_body(rows, out, pieces):
    width = rows.shape[1]
    piece = width // PARTS
    for q in range(PARTS):
        spread(pieces, q, rows[:, q * piece : (q + 1) * piece].astype(F32))
    flush(pieces, out, 0)


def pack(rows):
    total, width = rows.shape
    steps = 2
    piece = width // PARTS
    count = total // steps
    return call(
        pack_body,
        (steps,),
        [pl.BlockSpec((count, width), lambda i: (i, 0))],
        pl.BlockSpec((count * PARTS, piece), lambda i: (i, 0)),
        jax.ShapeDtypeStruct((total * PARTS, piece), BF16),
        (400 * total * width, 4 * total * width),
        [pltpu.VMEM((piece // LANES, count * PARTS, LANES), F32)],
    )(rows)


def combine_body(weighted, key, wgt, got, out, total, pieces):
    top, tok = key.shape
    step = pl.program_id(0)
    rows = got.shape[0] // PARTS
    piece = got.shape[1]
    mine = step * rows + lax.broadcasted_iota(jnp.int32, (rows, tok), 0)
    load = jnp.zeros((rows, tok), F32)
    for j in range(top):
        load = jnp.where(mine == key[j : j + 1, :], wgt[j : j + 1, :] if weighted else 1.0, load)
    high = load.astype(BF16)
    low = (load - high.astype(F32)).astype(BF16)
    fill(pieces, got)

    @pl.when(step == 0)
    def _():
        total[...] = jnp.zeros_like(total)

    for q in range(PARTS):
        lanes = slice(q * piece, (q + 1) * piece)
        part = collected(pieces, q, 0, piece)
        more = lax.dot_general(high, part, ROWS_BY_ROWS, preferred_element_type=F32)
        if weighted:
            more = more + lax.dot_general(low, part, ROWS_BY_ROWS, preferred_element_type=F32)
        total[:, lanes] += more

    @pl.when(step == pl.num_programs(0) - 1)
    def _():
        out[...] = total[...].astype(BF16)


def combine(key, wgt, got, weighted):
    top, tok = key.shape
    count, piece = got.shape
    steps = 2
    rows = count // steps
    return call(
        functools.partial(combine_body, weighted),
        (steps,),
        [whole((top, tok))] * 2 + [pl.BlockSpec((rows, piece), lambda i: (i, 0))],
        whole((tok, piece * PARTS)),
        jax.ShapeDtypeStruct((tok, piece * PARTS), BF16),
        (4 * count * tok * piece, 2 * count * piece),
        [pltpu.VMEM((tok, piece * PARTS), F32), pltpu.VMEM((piece // LANES, rows, LANES), F32)],
    )(key, wgt, got)


def exchange(x):
    return lax.all_to_all(x, AXES, split_axis=0, concat_axis=0, tiled=True)


def expert_forward(x, w_in, w_down):
    width = w_down.shape[0]
    projected = jnp.dot(x, w_in, preferred_element_type=F32)
    g, u = projected[:, :width], projected[:, width:]
    hidden = (g * jax.nn.sigmoid(g) * u).astype(BF16)
    return jnp.dot(hidden, w_down, preferred_element_type=F32).astype(BF16)


def expert_backward(x, cot, w_in, w_down):
    width = w_down.shape[0]
    projected = jnp.dot(x, w_in, preferred_element_type=F32)
    g, u = projected[:, :width], projected[:, width:]
    s = jax.nn.sigmoid(g)
    hidden = (g * s * u).astype(BF16)
    d_hidden = lax.dot_general(cot, w_down, COLS_BY_COLS, preferred_element_type=F32)
    d_gate = d_hidden * u * s * (1.0 + g * (1.0 - s))
    d_up = d_hidden * g * s
    d_proj = jnp.concatenate([d_gate, d_up], axis=1).astype(BF16)
    row_grad = lax.dot_general(
        d_proj, w_in, COLS_BY_COLS, preferred_element_type=F32
    ).astype(BF16)
    return row_grad, hidden, d_proj


def layer(
    tokens_fwd, experts_fwd, scores_fwd, tokens_bwd, experts_bwd, scores_bwd, cotangent, w_in, w_down
):
    devices = lax.axis_size("group") * lax.axis_size("inner")
    tok, top = experts_fwd.shape
    capacity = max(2, 3 * tok * top // (2 * devices))
    w_in, w_down = w_in[0], w_down[0]

    out_f, key_f, wgt_f = send(
        devices, capacity, experts_fwd.T, scores_fwd.T, (tokens_fwd,), (False,)
    )
    in_f = exchange(out_f)
    out_b, key_b, wgt_b = send(
        devices, capacity, experts_bwd.T, scores_bwd.T, (tokens_bwd, cotangent), (False, True)
    )
    out_b, in_f = lax.optimization_barrier((out_b, in_f))
    in_b = exchange(out_b)

    (rows_f,) = unpack(in_f, 1)
    back_f = pack(expert_forward(rows_f, w_in, w_down))
    back_f, in_b = lax.optimization_barrier((back_f, in_b))
    home_f = exchange(back_f)

    rows_b, cot_b = unpack(in_b, 2)
    row_grad, hidden, d_proj = expert_backward(rows_b, cot_b, w_in, w_down)
    back_b = pack(row_grad)
    back_b, home_f = lax.optimization_barrier((back_b, home_f))
    home_b = exchange(back_b)

    output_fwd = combine(key_f, wgt_f, home_f, True)
    grad_down = lax.dot_general(
        hidden, cot_b, ROWS_BY_ROWS, preferred_element_type=F32
    ).astype(BF16)
    grad_in = lax.dot_general(
        rows_b, d_proj, ROWS_BY_ROWS, preferred_element_type=F32
    ).astype(BF16)
    grad_tokens = combine(key_b, wgt_b, home_b, False)
    return output_fwd, grad_tokens, grad_in[None], grad_down[None]


def solution(mesh):
    rows = P(AXES, None)
    cube = P(AXES, None, None)
    return jax.shard_map(
        layer,
        mesh=mesh,
        in_specs=(rows,) * 7 + (cube,) * 2,
        out_specs=(rows, rows, cube, cube),
        check_vma=False,
    )
```

```python
import functools

import jax
import jax.numpy as jnp
from jax import lax
from jax.experimental import pallas as pl
from jax.experimental.pallas import tpu as pltpu
from jax.sharding import Mesh
from jax.sharding import PartitionSpec as P


FINE = ("y", "z", "x", "c")
TOP = 8
PARTS = 4
LANES = 128
F32 = jnp.float32
BF16 = jnp.bfloat16
ROWS_BY_ROWS = (((0,), (0,)), ((), ()))
COLS_BY_COLS = (((1,), (1,)), ((), ()))


def call(body, grid, in_specs, out_specs, out_shape, cost, scratch=()):
    return pl.pallas_call(
        body,
        grid=grid,
        in_specs=in_specs,
        out_specs=out_specs,
        out_shape=out_shape,
        scratch_shapes=list(scratch),
        compiler_params=pltpu.CompilerParams(
            dimension_semantics=("arbitrary",) * len(grid)
        ),
        cost_estimate=pl.CostEstimate(
            flops=cost[0], bytes_accessed=cost[1], transcendentals=0
        ),
    )


def whole(shape):
    return pl.BlockSpec(shape, lambda i: (0,) * len(shape))


def spread(pieces, q, rows):
    count, piece = rows.shape
    for k in range(piece // LANES):
        pieces[k, pl.ds(q, count, stride=PARTS), :] = rows[:, k * LANES : (k + 1) * LANES]


def collected(pieces, q, first, piece):
    count = pieces.shape[1] // PARTS
    return jnp.concatenate(
        [
            pieces[k, pl.ds(q, count, stride=PARTS), :]
            for k in range(first // LANES, (first + piece) // LANES)
        ],
        axis=1,
    ).astype(BF16)


def fill(pieces, chunks):
    for k in range(pieces.shape[0]):
        pieces[k] = chunks[:, k * LANES : (k + 1) * LANES].astype(F32)


def flush(pieces, out, first):
    for k in range(pieces.shape[0]):
        out[:, first + k * LANES : first + (k + 1) * LANES] = pieces[k].astype(BF16)


def place(experts, capacity, ids, sc, key, wgt):
    top, tok = ids.shape
    label = lax.broadcasted_iota(jnp.int32, (experts, tok), 0)
    hits = [label == ids[j : j + 1, :] for j in range(top)]
    chosen = jnp.zeros((experts, tok), F32)
    for hit in hits:
        chosen = jnp.where(hit, 1.0, chosen)
    earlier = lax.broadcasted_iota(jnp.int32, (tok, tok), 0) < lax.broadcasted_iota(
        jnp.int32, (tok, tok), 1
    )
    before = jnp.dot(
        chosen.astype(BF16),
        jnp.where(earlier, 1.0, 0.0).astype(BF16),
        preferred_element_type=F32,
    )
    for j in range(top):
        slot = jnp.sum(jnp.where(hits[j], before, 0.0), axis=0, keepdims=True)
        key[j : j + 1, :] = ids[j : j + 1, :] * capacity + slot.astype(jnp.int32)
    share = sc[...]
    wgt[...] = share / jnp.sum(share, axis=0, keepdims=True)


def payload_body(experts, capacity, ids, sc, *refs):
    *refs, key, wgt = refs
    tables, outs = refs[: len(refs) // 2], refs[len(refs) // 2 :]
    tok = ids.shape[1]
    place(experts, capacity, ids, sc, key, wgt)
    slot = key[...] - ids[...] * capacity
    share = wgt[...]
    first = share.astype(BF16)
    rest = share - first.astype(F32)
    second = rest.astype(BF16)
    third = (rest - second.astype(F32)).astype(BF16)
    facts = (ids[...].astype(F32), slot.astype(F32), first, second, third)
    for table, out in zip(tables, outs):
        out[:tok, :] = table[...]
        out[tok:, :] = jnp.zeros((out.shape[0] - tok, out.shape[1]), BF16)
        for k, fact in enumerate(facts):
            out[tok:, k * LANES : k * LANES + tok] = fact.astype(BF16)


def payload(experts, capacity, ids, sc, tables):
    tok, width = tables[0].shape
    n = len(tables)
    tall = (tok + ids.shape[0], width)
    return call(
        functools.partial(payload_body, experts, capacity),
        (1,),
        [whole(ids.shape)] * 2 + [whole((tok, width))] * n,
        [whole(tall)] * n + [whole(ids.shape)] * 2,
        [jax.ShapeDtypeStruct(tall, BF16)] * n
        + [jax.ShapeDtypeStruct(ids.shape, jnp.int32), jax.ShapeDtypeStruct(ids.shape, F32)],
        (50_000_000, 4 * n * tok * width),
    )(ids, sc, *tables)


def fact(pay, tok, k):
    return pay[tok:, k * LANES : k * LANES + tok].astype(F32)


def coordinates(ids):
    return ids >> 5, (ids >> 3) & 3, (ids >> 1) & 3, ids & 1


def plane_body(along, capacity, *refs):
    *pays, out, pieces = refs
    dests = out.shape[0]
    rows = dests * capacity
    tok = pays[0].shape[0] - TOP
    here = lax.axis_index(along)
    mine = pl.program_id(0) * rows + lax.broadcasted_iota(jnp.int32, (rows, tok), 0)
    for s, pay in enumerate(pays):
        ids = fact(pay, tok, 0).astype(jnp.int32)
        slot = fact(pay, tok, 1).astype(jnp.int32)
        y, z, x, c = coordinates(ids)
        near, far = (y, z) if along == "y" else (z, y)
        want = jnp.where(near == here, ((far * 4 + x) * 2 + c) * capacity + slot, -1)
        pick = jnp.zeros((rows, tok), F32)
        for j in range(TOP):
            pick = jnp.where(mine == want[j : j + 1, :], 1.0, pick)
        pick = pick.astype(BF16)
        piece = pay.shape[1] // PARTS
        for q in range(PARTS):
            got = jnp.dot(
                pick, pay[:tok, q * piece : (q + 1) * piece], preferred_element_type=F32
            )
            spread(pieces, q, got)
        for k in range(pieces.shape[0]):
            out[:, s, :, k * LANES : (k + 1) * LANES] = (
                pieces[k].reshape(dests, capacity * PARTS, LANES).astype(BF16)
            )


def plane(along, capacity, pays):
    tall, width = pays[0].shape
    steps = 2
    shape = (32, len(pays), capacity * PARTS, width // PARTS)
    return call(
        functools.partial(plane_body, along, capacity),
        (steps,),
        [whole((tall, width))] * len(pays),
        pl.BlockSpec((shape[0] // steps,) + shape[1:], lambda i: (i, 0, 0, 0)),
        jax.ShapeDtypeStruct(shape, BF16),
        (2_000_000_000, 8_000_000),
        [pltpu.VMEM((width // PARTS // LANES, 32 // steps * capacity * PARTS, LANES), F32)],
    )(*pays)


def rings_body(capacity, own, other, o0, o1, o2, o3, pieces):
    tall, width = own.shape[1:]
    tok = tall - TOP
    piece = width // PARTS
    rows = 16 * capacity
    my_y, my_z = lax.axis_index("y"), lax.axis_index("z")
    my_x, my_c = lax.axis_index("x"), lax.axis_index("c")
    mine = lax.broadcasted_iota(jnp.int32, (rows, tok), 0)
    for half, blocks in enumerate((own, other)):

        @pl.loop(0, blocks.shape[0])
        def _(i):
            pay = blocks.at[i]
            ids = fact(pay, tok, 0).astype(jnp.int32)
            slot = fact(pay, tok, 1).astype(jnp.int32)
            share = fact(pay, tok, 2) + fact(pay, tok, 3) + fact(pay, tok, 4)
            y, z, x, c = coordinates(ids)
            turn = ((y - my_y) & 3) * 4 + ((z - my_z) & 3)
            want = jnp.where((x == my_x) & (c == my_c), turn * capacity + slot, -1)
            pick = jnp.zeros((rows, tok), F32)
            load = jnp.zeros((rows, tok), F32)
            for j in range(TOP):
                hit = mine == want[j : j + 1, :]
                pick = jnp.where(hit, 1.0, pick)
                load = jnp.where(hit, share[j : j + 1, :], load)
            pick = pick.astype(BF16)
            scale = jnp.sum(load, axis=1, keepdims=True)
            for q in range(PARTS):
                got = jnp.dot(
                    pick, pay[:tok, q * piece : (q + 1) * piece], preferred_element_type=F32
                )
                spread(pieces, q, got * scale)
            for k in range(pieces.shape[0]):
                chunks = pieces[k].reshape(4, 4, capacity * PARTS, LANES).astype(BF16)
                for s, out in enumerate((o0, o1, o2, o3)):
                    out[:, half * 4 + i, :, k * LANES : (k + 1) * LANES] = chunks[s]


def rings(capacity, own, other):
    count, _, width = own.shape
    shape = (4, 2 * count, capacity * PARTS, width // PARTS)
    return call(
        functools.partial(rings_body, capacity),
        (1,),
        [whole(own.shape), whole(other.shape)],
        [whole(shape)] * 4,
        [jax.ShapeDtypeStruct(shape, BF16)] * 4,
        (2_000_000_000, 8_000_000),
        [pltpu.VMEM((width // PARTS // LANES, 16 * capacity * PARTS, LANES), F32)],
    )(own, other)


def regroup_body(*refs):
    parts, outs = refs[:4], refs[4:]
    for turn, out in enumerate(outs):
        for s, part in enumerate(parts):
            out[s] = part[turn]


def regroup(parts):
    shape = parts[0].shape
    return call(
        regroup_body,
        (1,),
        [whole(shape)] * 4,
        [whole(shape)] * 4,
        [jax.ShapeDtypeStruct(shape, BF16)] * 4,
        (1_000_000_000, 8_000_000),
    )(*parts)


def settle(pieces, source, pos):
    size = source.shape[0]
    start = pl.multiple_of(pos * size, 8)
    for k in range(pieces.shape[0]):
        pieces[k, pl.ds(start, size), :] = source[:, k * LANES : (k + 1) * LANES].astype(F32)


def lay_out(pieces, out):
    piece = out.shape[1] // PARTS
    for q in range(PARTS):
        out[:, q * piece : (q + 1) * piece] = collected(pieces, q, 0, piece)


def unplane_body(along, got, out, pieces):
    here = lax.axis_index(along)

    @pl.loop(0, got.shape[0])
    def _(d):
        for s in range(got.shape[1]):
            back = (here - s) & 3
            if along == "y":
                pos = back * 32 + d
            else:
                pos = (d >> 3) * 32 + back * 8 + (d & 7)
            settle(pieces, got.at[d, s], pos)

    lay_out(pieces, out)


def unrings_body(t0, t1, t2, t3, out, pieces):
    my_y, my_z = lax.axis_index("y"), lax.axis_index("z")
    my_x, my_c = lax.axis_index("x"), lax.axis_index("c")
    for turn, got in enumerate((t0, t1, t2, t3)):
        z = (my_z - turn) & 3

        @pl.loop(0, got.shape[0])
        def _(s):
            y = (my_y - s) & 3
            for b in range(got.shape[1]):
                x = (my_x - b % 4) & 3
                c = my_c if b < 4 else 1 - my_c
                settle(pieces, got.at[s, b], ((y * 4 + z) * 4 + x) * 2 + c)

    lay_out(pieces, out)


def rows_of(body, *got):
    _, piece = got[0].shape[-2:]
    total = sum(g.size for g in got) // piece
    return call(
        body,
        (1,),
        [whole(g.shape) for g in got],
        whole((total // PARTS, piece * PARTS)),
        jax.ShapeDtypeStruct((total // PARTS, piece * PARTS), BF16),
        (400 * total * piece, 4 * total * piece),
        [pltpu.VMEM((piece // LANES, total, LANES), F32)],
    )(*got)


def pack_body(rows, out, pieces):
    width = rows.shape[1]
    piece = width // PARTS
    for q in range(PARTS):
        spread(pieces, q, rows[:, q * piece : (q + 1) * piece].astype(F32))
    flush(pieces, out, 0)


def pack(rows):
    total, width = rows.shape
    steps = 2
    piece = width // PARTS
    count = total // steps
    return call(
        pack_body,
        (steps,),
        [pl.BlockSpec((count, width), lambda i: (i, 0))],
        pl.BlockSpec((count * PARTS, piece), lambda i: (i, 0)),
        jax.ShapeDtypeStruct((total * PARTS, piece), BF16),
        (400 * total * width, 4 * total * width),
        [pltpu.VMEM((piece // LANES, count * PARTS, LANES), F32)],
    )(rows)


def combine_body(weighted, key, wgt, got, out, total, pieces):
    top, tok = key.shape
    step = pl.program_id(0)
    rows = got.shape[0] // PARTS
    piece = got.shape[1]
    mine = step * rows + lax.broadcasted_iota(jnp.int32, (rows, tok), 0)
    load = jnp.zeros((rows, tok), F32)
    for j in range(top):
        load = jnp.where(mine == key[j : j + 1, :], wgt[j : j + 1, :] if weighted else 1.0, load)
    high = load.astype(BF16)
    low = (load - high.astype(F32)).astype(BF16)
    fill(pieces, got)

    @pl.when(step == 0)
    def _():
        total[...] = jnp.zeros_like(total)

    for q in range(PARTS):
        lanes = slice(q * piece, (q + 1) * piece)
        part = collected(pieces, q, 0, piece)
        more = lax.dot_general(high, part, ROWS_BY_ROWS, preferred_element_type=F32)
        if weighted:
            more = more + lax.dot_general(low, part, ROWS_BY_ROWS, preferred_element_type=F32)
        total[:, lanes] += more

    @pl.when(step == pl.num_programs(0) - 1)
    def _():
        out[...] = total[...].astype(BF16)


def combine(key, wgt, got, weighted):
    top, tok = key.shape
    count, piece = got.shape
    steps = 2
    rows = count // steps
    return call(
        functools.partial(combine_body, weighted),
        (steps,),
        [whole((top, tok))] * 2 + [pl.BlockSpec((rows, piece), lambda i: (i, 0))],
        whole((tok, piece * PARTS)),
        jax.ShapeDtypeStruct((tok, piece * PARTS), BF16),
        (4 * count * tok * piece, 2 * count * piece),
        [pltpu.VMEM((tok, piece * PARTS), F32), pltpu.VMEM((piece // LANES, rows, LANES), F32)],
    )(key, wgt, got)


def exchange(x, axes=FINE):
    return lax.all_to_all(x, axes, split_axis=0, concat_axis=0, tiled=True)


def turned(x, axis, turn):
    return lax.ppermute(x, axis, [(i, (i + turn) % 4) for i in range(4)])


def gathered(x, axis):
    return [x] + [turned(x, axis, turn) for turn in (1, 3, 2)]


def in_order(parts):
    return [parts[0], parts[1], parts[3], parts[2]]


def expert_forward(x, w_in, w_down):
    width = w_down.shape[0]
    projected = jnp.dot(x, w_in, preferred_element_type=F32)
    g, u = projected[:, :width], projected[:, width:]
    hidden = (g * jax.nn.sigmoid(g) * u).astype(BF16)
    return jnp.dot(hidden, w_down, preferred_element_type=F32).astype(BF16)


def expert_backward(projected, cot, w_in, w_down):
    width = w_down.shape[0]
    g, u = projected[:, :width], projected[:, width:]
    s = jax.nn.sigmoid(g)
    hidden = (g * s * u).astype(BF16)
    d_hidden = lax.dot_general(cot, w_down, COLS_BY_COLS, preferred_element_type=F32)
    d_gate = d_hidden * u * s * (1.0 + g * (1.0 - s))
    d_up = d_hidden * g * s
    d_proj = jnp.concatenate([d_gate, d_up], axis=1).astype(BF16)
    row_grad = lax.dot_general(
        d_proj, w_in, COLS_BY_COLS, preferred_element_type=F32
    ).astype(BF16)
    return row_grad, hidden, d_proj


def layer(
    tokens_fwd, experts_fwd, scores_fwd, tokens_bwd, experts_bwd, scores_bwd, cotangent, w_in, w_down
):
    devices = lax.axis_size(FINE)
    tok, top = experts_fwd.shape
    capacity = max(2, 3 * tok * top // (2 * devices))
    w_in, w_down = w_in[0], w_down[0]

    pay_f, key_f, wgt_f = payload(
        devices, capacity, experts_fwd.T, scores_fwd.T, (tokens_fwd,)
    )
    near_f = in_order(gathered(pay_f, "y"))
    pay_b, pay_c, key_b, wgt_b = payload(
        devices, capacity, experts_bwd.T, scores_bwd.T, (tokens_bwd, cotangent)
    )
    near_c = in_order(gathered(pay_c, "x"))
    near_b = in_order(gathered(pay_b, "z"))

    out_f = plane("y", capacity, near_f)
    in_f = exchange(out_f, ("z", "x", "c"))

    own_c = jnp.stack(near_c)
    other_c = lax.ppermute(own_c, "c", [(0, 1), (1, 0)])
    out_c = rings(capacity, own_c, other_c)
    by_y = [out_c[0]] + [turned(out_c[s], "y", s) for s in (1, 2, 3)]
    out_b = plane("z", capacity, near_b)
    out_b, in_f = lax.optimization_barrier((out_b, in_f))
    in_b = exchange(out_b, ("y", "x", "c"))

    rows_f = rows_of(functools.partial(unplane_body, "y"), in_f)
    by_z = regroup(by_y)
    in_c = [by_z[0]] + [turned(by_z[turn], "z", turn) for turn in (1, 2, 3)]
    out_rows = expert_forward(rows_f, w_in, w_down)
    back_f = pack(out_rows)
    back_f, in_b = lax.optimization_barrier((back_f, in_b))
    home_f = exchange(back_f)

    rows_b = rows_of(functools.partial(unplane_body, "z"), in_b)
    projected = jnp.dot(rows_b, w_in, preferred_element_type=F32)
    cot_b = rows_of(unrings_body, *in_c)
    row_grad, hidden, d_proj = expert_backward(projected, cot_b, w_in, w_down)
    back_b = pack(row_grad)
    back_b, home_f = lax.optimization_barrier((back_b, home_f))
    home_b = exchange(back_b)

    output_fwd = combine(key_f, wgt_f, home_f, True)
    grad_down = lax.dot_general(
        hidden, cot_b, ROWS_BY_ROWS, preferred_element_type=F32
    ).astype(BF16)
    grad_in = lax.dot_general(
        rows_b, d_proj, ROWS_BY_ROWS, preferred_element_type=F32
    ).astype(BF16)
    grad_tokens = combine(key_b, wgt_b, home_b, False)
    return output_fwd, grad_tokens, grad_in[None], grad_down[None]


def solution(mesh):
    rows = P(FINE, None)
    cube = P(FINE, None, None)
    fine = Mesh(mesh.devices.reshape(4, 4, 4, 2), FINE)
    return jax.shard_map(
        layer,
        mesh=fine,
        in_specs=(rows,) * 7 + (cube,) * 2,
        out_specs=(rows, rows, cube, cube),
        check_vma=False,
    )
```

```python
import functools

import jax
import jax.numpy as jnp
from jax import lax
from jax.experimental import pallas as pl
from jax.experimental.pallas import tpu as pltpu
from jax.sharding import Mesh
from jax.sharding import PartitionSpec as P


FINE = ("y", "z", "x", "c")
TOP = 8
PARTS = 4
LANES = 128
F32 = jnp.float32
BF16 = jnp.bfloat16
ROWS_BY_ROWS = (((0,), (0,)), ((), ()))
COLS_BY_COLS = (((1,), (1,)), ((), ()))


def call(body, grid, in_specs, out_specs, out_shape, cost, scratch=()):
    return pl.pallas_call(
        body,
        grid=grid,
        in_specs=in_specs,
        out_specs=out_specs,
        out_shape=out_shape,
        scratch_shapes=list(scratch),
        compiler_params=pltpu.CompilerParams(
            dimension_semantics=("arbitrary",) * len(grid)
        ),
        cost_estimate=pl.CostEstimate(
            flops=cost[0], bytes_accessed=cost[1], transcendentals=0
        ),
    )


def whole(shape):
    return pl.BlockSpec(shape, lambda i: (0,) * len(shape))


def spread(pieces, q, rows):
    count, piece = rows.shape
    for k in range(piece // LANES):
        pieces[k, pl.ds(q, count, stride=PARTS), :] = rows[:, k * LANES : (k + 1) * LANES]


def collected(pieces, q, first, piece):
    count = pieces.shape[1] // PARTS
    return jnp.concatenate(
        [
            pieces[k, pl.ds(q, count, stride=PARTS), :]
            for k in range(first // LANES, (first + piece) // LANES)
        ],
        axis=1,
    ).astype(BF16)


def fill(pieces, chunks):
    for k in range(pieces.shape[0]):
        pieces[k] = chunks[:, k * LANES : (k + 1) * LANES].astype(F32)


def place(experts, capacity, ids, sc, key, wgt):
    top, tok = ids.shape
    label = lax.broadcasted_iota(jnp.int32, (experts, tok), 0)
    hits = [label == ids[j : j + 1, :] for j in range(top)]
    chosen = jnp.zeros((experts, tok), F32)
    for hit in hits:
        chosen = jnp.where(hit, 1.0, chosen)
    earlier = lax.broadcasted_iota(jnp.int32, (tok, tok), 0) < lax.broadcasted_iota(
        jnp.int32, (tok, tok), 1
    )
    before = jnp.dot(
        chosen.astype(BF16),
        jnp.where(earlier, 1.0, 0.0).astype(BF16),
        preferred_element_type=F32,
    )
    for j in range(top):
        slot = jnp.sum(jnp.where(hits[j], before, 0.0), axis=0, keepdims=True)
        key[j : j + 1, :] = ids[j : j + 1, :] * capacity + slot.astype(jnp.int32)
    share = sc[...]
    wgt[...] = share / jnp.sum(share, axis=0, keepdims=True)


def payload_body(experts, capacity, ids, sc, *refs):
    *refs, key, wgt = refs
    tables, outs = refs[: len(refs) // 2], refs[len(refs) // 2 :]
    tok = ids.shape[1]
    place(experts, capacity, ids, sc, key, wgt)
    slot = key[...] - ids[...] * capacity
    share = wgt[...]
    first = share.astype(BF16)
    rest = share - first.astype(F32)
    second = rest.astype(BF16)
    third = (rest - second.astype(F32)).astype(BF16)
    facts = (ids[...].astype(F32), slot.astype(F32), first, second, third)
    for table, out in zip(tables, outs):
        out[:tok, :] = table[...]
        out[tok:, :] = jnp.zeros((out.shape[0] - tok, out.shape[1]), BF16)
        for k, fact in enumerate(facts):
            out[tok:, k * LANES : k * LANES + tok] = fact.astype(BF16)


def payload(experts, capacity, ids, sc, tables):
    tok, width = tables[0].shape
    n = len(tables)
    tall = (tok + ids.shape[0], width)
    return call(
        functools.partial(payload_body, experts, capacity),
        (1,),
        [whole(ids.shape)] * 2 + [whole((tok, width))] * n,
        [whole(tall)] * n + [whole(ids.shape)] * 2,
        [jax.ShapeDtypeStruct(tall, BF16)] * n
        + [jax.ShapeDtypeStruct(ids.shape, jnp.int32), jax.ShapeDtypeStruct(ids.shape, F32)],
        (50_000_000, 4 * n * tok * width),
    )(ids, sc, *tables)


def fact(pay, tok, k):
    return pay[tok:, k * LANES : k * LANES + tok].astype(F32)


def coordinates(ids):
    return ids >> 5, (ids >> 3) & 3, (ids >> 1) & 3, ids & 1


def plane_body(along, capacity, *refs):
    *pays, out = refs
    rows, width = out.shape
    tok = pays[0].shape[0] - TOP
    here = lax.axis_index(along)
    mine = pl.program_id(0) * rows + lax.broadcasted_iota(jnp.int32, (rows, tok), 0)
    picks = []
    for s, pay in enumerate(pays):
        ids = fact(pay, tok, 0).astype(jnp.int32)
        slot = fact(pay, tok, 1).astype(jnp.int32)
        y, z, x, c = coordinates(ids)
        near, far = (y, z) if along == "y" else (z, y)
        place_of = ((far * 4 + x) * 2 + c) * len(pays) + s
        want = jnp.where(near == here, place_of * capacity + slot, -1)
        pick = jnp.zeros((rows, tok), F32)
        for j in range(TOP):
            pick = jnp.where(mine == want[j : j + 1, :], 1.0, pick)
        picks.append(pick.astype(BF16))
    piece = width // PARTS
    for q in range(PARTS):
        lanes = slice(q * piece, (q + 1) * piece)
        got = jnp.zeros((rows, piece), F32)
        for pick, pay in zip(picks, pays):
            got = got + jnp.dot(pick, pay[:tok, lanes], preferred_element_type=F32)
        out[:, lanes] = got.astype(BF16)


def plane(along, capacity, pays):
    tall, width = pays[0].shape
    steps = 2
    rows = 32 * len(pays) * capacity
    return call(
        functools.partial(plane_body, along, capacity),
        (steps,),
        [whole((tall, width))] * len(pays),
        pl.BlockSpec((rows // steps, width), lambda i: (i, 0)),
        jax.ShapeDtypeStruct((rows, width), BF16),
        (2_000_000_000, 8_000_000),
    )(*pays)


def rings_body(capacity, own, other, o0, o1, o2, o3, pieces):
    tall, width = own.shape[1:]
    tok = tall - TOP
    piece = width // PARTS
    rows = 16 * capacity
    my_y, my_z = lax.axis_index("y"), lax.axis_index("z")
    my_x, my_c = lax.axis_index("x"), lax.axis_index("c")
    mine = lax.broadcasted_iota(jnp.int32, (rows, tok), 0)
    for half, blocks in enumerate((own, other)):

        @pl.loop(0, blocks.shape[0])
        def _(i):
            pay = blocks.at[i]
            ids = fact(pay, tok, 0).astype(jnp.int32)
            slot = fact(pay, tok, 1).astype(jnp.int32)
            share = fact(pay, tok, 2) + fact(pay, tok, 3) + fact(pay, tok, 4)
            y, z, x, c = coordinates(ids)
            turn = ((y - my_y) & 3) * 4 + ((z - my_z) & 3)
            want = jnp.where((x == my_x) & (c == my_c), turn * capacity + slot, -1)
            pick = jnp.zeros((rows, tok), F32)
            load = jnp.zeros((rows, tok), F32)
            for j in range(TOP):
                hit = mine == want[j : j + 1, :]
                pick = jnp.where(hit, 1.0, pick)
                load = jnp.where(hit, share[j : j + 1, :], load)
            pick = pick.astype(BF16)
            scale = jnp.sum(load, axis=1, keepdims=True)
            for q in range(PARTS):
                got = jnp.dot(
                    pick, pay[:tok, q * piece : (q + 1) * piece], preferred_element_type=F32
                )
                spread(pieces, q, got * scale)
            for k in range(pieces.shape[0]):
                chunks = pieces[k].reshape(4, 4, capacity * PARTS, LANES).astype(BF16)
                for s, out in enumerate((o0, o1, o2, o3)):
                    out[:, half * 4 + i, :, k * LANES : (k + 1) * LANES] = chunks[s]


def rings(capacity, own, other):
    count, _, width = own.shape
    shape = (4, 2 * count, capacity * PARTS, width // PARTS)
    return call(
        functools.partial(rings_body, capacity),
        (1,),
        [whole(own.shape), whole(other.shape)],
        [whole(shape)] * 4,
        [jax.ShapeDtypeStruct(shape, BF16)] * 4,
        (2_000_000_000, 8_000_000),
        [pltpu.VMEM((width // PARTS // LANES, 16 * capacity * PARTS, LANES), F32)],
    )(own, other)


def regroup_body(*refs):
    parts, outs = refs[:4], refs[4:]
    for turn, out in enumerate(outs):
        for s, part in enumerate(parts):
            out[s] = part[turn]


def regroup(parts):
    shape = parts[0].shape
    return call(
        regroup_body,
        (1,),
        [whole(shape)] * 4,
        [whole(shape)] * 4,
        [jax.ShapeDtypeStruct(shape, BF16)] * 4,
        (1_000_000_000, 8_000_000),
    )(*parts)


def settle(pieces, source, pos):
    size = source.shape[0]
    start = pl.multiple_of(pos * size, 8)
    for k in range(pieces.shape[0]):
        pieces[k, pl.ds(start, size), :] = source[:, k * LANES : (k + 1) * LANES].astype(F32)


def lay_out(pieces, out):
    piece = out.shape[1] // PARTS
    for q in range(PARTS):
        out[:, q * piece : (q + 1) * piece] = collected(pieces, q, 0, piece)


def unrings_body(t0, t1, t2, t3, out, pieces):
    my_y, my_x, my_c = lax.axis_index("y"), lax.axis_index("x"), lax.axis_index("c")
    for turn, got in enumerate((t0, t1, t2, t3)):

        @pl.loop(0, got.shape[0])
        def _(s):
            y = (my_y - s) & 3
            for b in range(got.shape[1]):
                x = (my_x - b % 4) & 3
                c = my_c if b < 4 else 1 - my_c
                settle(pieces, got.at[s, b], ((y * 4 + x) * 2 + c) * 4 + turn)

    lay_out(pieces, out)


def rows_of(body, *got):
    _, piece = got[0].shape[-2:]
    total = sum(g.size for g in got) // piece
    return call(
        body,
        (1,),
        [whole(g.shape) for g in got],
        whole((total // PARTS, piece * PARTS)),
        jax.ShapeDtypeStruct((total // PARTS, piece * PARTS), BF16),
        (400 * total * piece, 4 * total * piece),
        [pltpu.VMEM((piece // LANES, total, LANES), F32)],
    )(*got)


def pack_body(along, rows, out, pieces):
    piece = rows.shape[1] // PARTS
    size = out.shape[1]
    here = lax.axis_index(along)
    for q in range(PARTS):
        spread(pieces, q, rows[:, q * piece : (q + 1) * piece].astype(F32))

    @pl.loop(0, out.shape[0] // 4)
    def _(d):
        for s in range(4):
            back = (here - s) & 3
            if along == "y":
                pos = back * 32 + d
            else:
                pos = (d >> 3) * 32 + back * 8 + (d & 7)
            start = pl.multiple_of((d * 4 + s) * size, 8)
            for k in range(pieces.shape[0]):
                out[pos, :, k * LANES : (k + 1) * LANES] = pieces[
                    k, pl.ds(start, size), :
                ].astype(BF16)


def pack(along, capacity, rows):
    total, width = rows.shape
    piece = width // PARTS
    shape = (total // capacity, capacity * PARTS, piece)
    return call(
        functools.partial(pack_body, along),
        (1,),
        [whole((total, width))],
        whole(shape),
        jax.ShapeDtypeStruct(shape, BF16),
        (400 * total * width, 4 * total * width),
        [pltpu.VMEM((piece // LANES, total * PARTS, LANES), F32)],
    )(rows).reshape(total * PARTS, piece)


def combine_body(weighted, key, wgt, got, out, total, pieces):
    top, tok = key.shape
    step = pl.program_id(0)
    rows = got.shape[0] // PARTS
    piece = got.shape[1]
    mine = step * rows + lax.broadcasted_iota(jnp.int32, (rows, tok), 0)
    load = jnp.zeros((rows, tok), F32)
    for j in range(top):
        load = jnp.where(mine == key[j : j + 1, :], wgt[j : j + 1, :] if weighted else 1.0, load)
    high = load.astype(BF16)
    low = (load - high.astype(F32)).astype(BF16)
    fill(pieces, got)

    @pl.when(step == 0)
    def _():
        total[...] = jnp.zeros_like(total)

    for q in range(PARTS):
        lanes = slice(q * piece, (q + 1) * piece)
        part = collected(pieces, q, 0, piece)
        more = lax.dot_general(high, part, ROWS_BY_ROWS, preferred_element_type=F32)
        if weighted:
            more = more + lax.dot_general(low, part, ROWS_BY_ROWS, preferred_element_type=F32)
        total[:, lanes] += more

    @pl.when(step == pl.num_programs(0) - 1)
    def _():
        out[...] = total[...].astype(BF16)


def combine(key, wgt, got, weighted):
    top, tok = key.shape
    count, piece = got.shape
    steps = 2
    rows = count // steps
    return call(
        functools.partial(combine_body, weighted),
        (steps,),
        [whole((top, tok))] * 2 + [pl.BlockSpec((rows, piece), lambda i: (i, 0))],
        whole((tok, piece * PARTS)),
        jax.ShapeDtypeStruct((tok, piece * PARTS), BF16),
        (4 * count * tok * piece, 2 * count * piece),
        [pltpu.VMEM((tok, piece * PARTS), F32), pltpu.VMEM((piece // LANES, rows, LANES), F32)],
    )(key, wgt, got)


def exchange(x, axes=FINE):
    return lax.all_to_all(x, axes, split_axis=0, concat_axis=0, tiled=True)


def turned(x, axis, turn):
    return lax.ppermute(x, axis, [(i, (i + turn) % 4) for i in range(4)])


def gathered(x, axis):
    return [x] + [turned(x, axis, turn) for turn in (1, 3, 2)]


def in_order(parts):
    return [parts[0], parts[1], parts[3], parts[2]]


def expert_forward(x, w_in, w_down):
    width = w_down.shape[0]
    projected = jnp.dot(x, w_in, preferred_element_type=F32)
    g, u = projected[:, :width], projected[:, width:]
    hidden = (g * jax.nn.sigmoid(g) * u).astype(BF16)
    return jnp.dot(hidden, w_down, preferred_element_type=F32).astype(BF16)


def expert_backward(projected, cot, w_in, w_down):
    width = w_down.shape[0]
    g, u = projected[:, :width], projected[:, width:]
    s = jax.nn.sigmoid(g)
    hidden = (g * s * u).astype(BF16)
    d_hidden = lax.dot_general(cot, w_down, COLS_BY_COLS, preferred_element_type=F32)
    d_gate = d_hidden * u * s * (1.0 + g * (1.0 - s))
    d_up = d_hidden * g * s
    d_proj = jnp.concatenate([d_gate, d_up], axis=1).astype(BF16)
    row_grad = lax.dot_general(
        d_proj, w_in, COLS_BY_COLS, preferred_element_type=F32
    ).astype(BF16)
    return row_grad, hidden, d_proj


def layer(
    tokens_fwd, experts_fwd, scores_fwd, tokens_bwd, experts_bwd, scores_bwd, cotangent, w_in, w_down
):
    devices = lax.axis_size(FINE)
    tok, top = experts_fwd.shape
    capacity = max(2, 3 * tok * top // (2 * devices))
    w_in, w_down = w_in[0], w_down[0]

    pay_f, key_f, wgt_f = payload(
        devices, capacity, experts_fwd.T, scores_fwd.T, (tokens_fwd,)
    )
    near_f = in_order(gathered(pay_f, "y"))
    pay_b, pay_c, key_b, wgt_b = payload(
        devices, capacity, experts_bwd.T, scores_bwd.T, (tokens_bwd, cotangent)
    )
    near_c = in_order(gathered(pay_c, "x"))
    near_b = in_order(gathered(pay_b, "z"))

    out_f = plane("y", capacity, near_f)
    in_f = exchange(out_f, ("z", "x", "c"))

    own_c = jnp.stack(near_c)
    other_c = lax.ppermute(own_c, "c", [(0, 1), (1, 0)])
    out_c = rings(capacity, own_c, other_c)
    by_y = [out_c[0]] + [turned(out_c[s], "y", s) for s in (1, 2, 3)]
    out_b = plane("z", capacity, near_b)
    out_b, in_f = lax.optimization_barrier((out_b, in_f))
    in_b = exchange(out_b, ("y", "x", "c"))

    by_z = regroup(by_y)
    in_c = [by_z[0]] + [turned(by_z[turn], "z", turn) for turn in (1, 2, 3)]
    out_rows = expert_forward(in_f, w_in, w_down)
    back_f = pack("y", capacity, out_rows)
    back_f, in_b = lax.optimization_barrier((back_f, in_b))
    home_f = exchange(back_f)

    rows_b = in_b
    projected = jnp.dot(rows_b, w_in, preferred_element_type=F32)
    cot_b = rows_of(unrings_body, *in_c)
    row_grad, hidden, d_proj = expert_backward(projected, cot_b, w_in, w_down)
    back_b = pack("z", capacity, row_grad)
    back_b, home_f = lax.optimization_barrier((back_b, home_f))
    home_b = exchange(back_b)

    output_fwd = combine(key_f, wgt_f, home_f, True)
    grad_down = lax.dot_general(
        hidden, cot_b, ROWS_BY_ROWS, preferred_element_type=F32
    ).astype(BF16)
    grad_in = lax.dot_general(
        rows_b, d_proj, ROWS_BY_ROWS, preferred_element_type=F32
    ).astype(BF16)
    grad_tokens = combine(key_b, wgt_b, home_b, False)
    return output_fwd, grad_tokens, grad_in[None], grad_down[None]


def solution(mesh):
    rows = P(FINE, None)
    cube = P(FINE, None, None)
    fine = Mesh(mesh.devices.reshape(4, 4, 4, 2), FINE)
    return jax.shard_map(
        layer,
        mesh=fine,
        in_specs=(rows,) * 7 + (cube,) * 2,
        out_specs=(rows, rows, cube, cube),
        check_vma=False,
    )
```

```python
import functools

import jax
import jax.numpy as jnp
from jax import lax
from jax.experimental import pallas as pl
from jax.experimental.pallas import tpu as pltpu
from jax.sharding import Mesh
from jax.sharding import PartitionSpec as P


FINE = ("y", "z", "x", "c")
TOP = 8
PARTS = 4
LANES = 128
F32 = jnp.float32
BF16 = jnp.bfloat16
ROWS_BY_ROWS = (((0,), (0,)), ((), ()))
COLS_BY_COLS = (((1,), (1,)), ((), ()))


def call(body, grid, in_specs, out_specs, out_shape, cost, scratch=()):
    return pl.pallas_call(
        body,
        grid=grid,
        in_specs=in_specs,
        out_specs=out_specs,
        out_shape=out_shape,
        scratch_shapes=list(scratch),
        compiler_params=pltpu.CompilerParams(
            dimension_semantics=("arbitrary",) * len(grid)
        ),
        cost_estimate=pl.CostEstimate(
            flops=cost[0], bytes_accessed=cost[1], transcendentals=0
        ),
    )


def whole(shape):
    return pl.BlockSpec(shape, lambda i: (0,) * len(shape))


def spread(pieces, q, rows):
    count, piece = rows.shape
    for k in range(piece // LANES):
        pieces[k, pl.ds(q, count, stride=PARTS), :] = rows[:, k * LANES : (k + 1) * LANES]


def collected(pieces, q, first, piece):
    count = pieces.shape[1] // PARTS
    return jnp.concatenate(
        [
            pieces[k, pl.ds(q, count, stride=PARTS), :]
            for k in range(first // LANES, (first + piece) // LANES)
        ],
        axis=1,
    ).astype(BF16)


def fill(pieces, chunks):
    for k in range(pieces.shape[0]):
        pieces[k] = chunks[:, k * LANES : (k + 1) * LANES].astype(F32)


def place(experts, capacity, ids, sc, key, wgt):
    top, tok = ids.shape
    label = lax.broadcasted_iota(jnp.int32, (experts, tok), 0)
    hits = [label == ids[j : j + 1, :] for j in range(top)]
    chosen = jnp.zeros((experts, tok), F32)
    for hit in hits:
        chosen = jnp.where(hit, 1.0, chosen)
    earlier = lax.broadcasted_iota(jnp.int32, (tok, tok), 0) < lax.broadcasted_iota(
        jnp.int32, (tok, tok), 1
    )
    before = jnp.dot(
        chosen.astype(BF16),
        jnp.where(earlier, 1.0, 0.0).astype(BF16),
        preferred_element_type=F32,
    )
    for j in range(top):
        slot = jnp.sum(jnp.where(hits[j], before, 0.0), axis=0, keepdims=True)
        key[j : j + 1, :] = ids[j : j + 1, :] * capacity + slot.astype(jnp.int32)
    share = sc[...]
    wgt[...] = share / jnp.sum(share, axis=0, keepdims=True)


def payload_body(experts, capacity, ids, sc, *refs):
    *refs, key, wgt = refs
    tables, outs = refs[: len(refs) // 2], refs[len(refs) // 2 :]
    tok = ids.shape[1]
    place(experts, capacity, ids, sc, key, wgt)
    slot = key[...] - ids[...] * capacity
    share = wgt[...]
    first = share.astype(BF16)
    rest = share - first.astype(F32)
    second = rest.astype(BF16)
    third = (rest - second.astype(F32)).astype(BF16)
    facts = (ids[...].astype(F32), slot.astype(F32), first, second, third)
    for table, out in zip(tables, outs):
        out[:tok, :] = table[...]
        out[tok:, :] = jnp.zeros((out.shape[0] - tok, out.shape[1]), BF16)
        for k, fact in enumerate(facts):
            out[tok:, k * LANES : k * LANES + tok] = fact.astype(BF16)


def payload(experts, capacity, ids, sc, tables):
    tok, width = tables[0].shape
    n = len(tables)
    tall = (tok + ids.shape[0], width)
    return call(
        functools.partial(payload_body, experts, capacity),
        (1,),
        [whole(ids.shape)] * 2 + [whole((tok, width))] * n,
        [whole(tall)] * n + [whole(ids.shape)] * 2,
        [jax.ShapeDtypeStruct(tall, BF16)] * n
        + [jax.ShapeDtypeStruct(ids.shape, jnp.int32), jax.ShapeDtypeStruct(ids.shape, F32)],
        (50_000_000, 4 * n * tok * width),
    )(ids, sc, *tables)


def fact(pay, tok, k):
    return pay[tok:, k * LANES : k * LANES + tok].astype(F32)


def coordinates(ids):
    return ids >> 5, (ids >> 3) & 3, (ids >> 1) & 3, ids & 1


def plane_body(along, capacity, *refs):
    *pays, out, want, table = refs
    rows, _ = out.shape
    tok = pays[0].shape[0] - TOP
    here = lax.axis_index(along)

    @pl.when(pl.program_id(0) == 0)
    def _():
        for s, pay in enumerate(pays):
            ids = fact(pay, tok, 0).astype(jnp.int32)
            slot = fact(pay, tok, 1).astype(jnp.int32)
            y, z, x, c = coordinates(ids)
            near, far = (y, z) if along == "y" else (z, y)
            place_of = ((far * 4 + x) * 2 + c) * len(pays) + s
            want[:, s * tok : (s + 1) * tok] = jnp.where(
                near == here, place_of * capacity + slot, -1
            )
            table[s * tok : (s + 1) * tok, :] = pay[:tok, :]

    wide = want.shape[1]
    mine = pl.program_id(0) * rows + lax.broadcasted_iota(jnp.int32, (rows, wide), 0)
    pick = jnp.zeros((rows, wide), F32)
    for j in range(TOP):
        pick = jnp.where(mine == want[j : j + 1, :], 1.0, pick)
    out[...] = jnp.dot(pick.astype(BF16), table[...], preferred_element_type=F32).astype(BF16)


def plane(along, capacity, pays):
    tall, width = pays[0].shape
    steps = 2
    rows = 32 * len(pays) * capacity
    return call(
        functools.partial(plane_body, along, capacity),
        (steps,),
        [whole((tall, width))] * len(pays),
        pl.BlockSpec((rows // steps, width), lambda i: (i, 0)),
        jax.ShapeDtypeStruct((rows, width), BF16),
        (2_000_000_000, 8_000_000),
        [
            pltpu.VMEM((TOP, len(pays) * (tall - TOP)), jnp.int32),
            pltpu.VMEM((len(pays) * (tall - TOP), width), BF16),
        ],
    )(*pays)


def rings_body(capacity, own, other, o0, o1, o2, o3, pieces):
    tall, width = own.shape[1:]
    tok = tall - TOP
    piece = width // PARTS
    rows = 16 * capacity
    my_y, my_z = lax.axis_index("y"), lax.axis_index("z")
    my_x, my_c = lax.axis_index("x"), lax.axis_index("c")
    mine = lax.broadcasted_iota(jnp.int32, (rows, tok), 0)
    for half, blocks in enumerate((own, other)):

        @pl.loop(0, blocks.shape[0])
        def _(i):
            pay = blocks.at[i]
            ids = fact(pay, tok, 0).astype(jnp.int32)
            slot = fact(pay, tok, 1).astype(jnp.int32)
            share = fact(pay, tok, 2) + fact(pay, tok, 3) + fact(pay, tok, 4)
            y, z, x, c = coordinates(ids)
            turn = ((y - my_y) & 3) * 4 + ((z - my_z) & 3)
            want = jnp.where((x == my_x) & (c == my_c), turn * capacity + slot, -1)
            pick = jnp.zeros((rows, tok), F32)
            load = jnp.zeros((rows, tok), F32)
            for j in range(TOP):
                hit = mine == want[j : j + 1, :]
                pick = jnp.where(hit, 1.0, pick)
                load = jnp.where(hit, share[j : j + 1, :], load)
            pick = pick.astype(BF16)
            scale = jnp.sum(load, axis=1, keepdims=True)
            for q in range(PARTS):
                got = jnp.dot(
                    pick, pay[:tok, q * piece : (q + 1) * piece], preferred_element_type=F32
                )
                spread(pieces, q, got * scale)
            for k in range(pieces.shape[0]):
                chunks = pieces[k].reshape(4, 4, capacity * PARTS, LANES).astype(BF16)
                for s, out in enumerate((o0, o1, o2, o3)):
                    out[:, half * 4 + i, :, k * LANES : (k + 1) * LANES] = chunks[s]


def rings(capacity, own, other):
    count, _, width = own.shape
    shape = (4, 2 * count, capacity * PARTS, width // PARTS)
    return call(
        functools.partial(rings_body, capacity),
        (1,),
        [whole(own.shape), whole(other.shape)],
        [whole(shape)] * 4,
        [jax.ShapeDtypeStruct(shape, BF16)] * 4,
        (2_000_000_000, 8_000_000),
        [pltpu.VMEM((width // PARTS // LANES, 16 * capacity * PARTS, LANES), F32)],
    )(own, other)


def regroup_body(*refs):
    parts, outs = refs[:4], refs[4:]
    for turn, out in enumerate(outs):
        for s, part in enumerate(parts):
            out[s] = part[turn]


def regroup(parts):
    shape = parts[0].shape
    return call(
        regroup_body,
        (1,),
        [whole(shape)] * 4,
        [whole(shape)] * 4,
        [jax.ShapeDtypeStruct(shape, BF16)] * 4,
        (1_000_000_000, 8_000_000),
    )(*parts)


def settle(pieces, source, pos):
    size = source.shape[0]
    start = pl.multiple_of(pos * size, 8)
    for k in range(pieces.shape[0]):
        pieces[k, pl.ds(start, size), :] = source[:, k * LANES : (k + 1) * LANES].astype(F32)


def lay_out(pieces, out):
    piece = out.shape[1] // PARTS
    for q in range(PARTS):
        out[:, q * piece : (q + 1) * piece] = collected(pieces, q, 0, piece)


def unrings_body(t0, t1, t2, t3, out, pieces):
    my_y, my_x, my_c = lax.axis_index("y"), lax.axis_index("x"), lax.axis_index("c")
    for turn, got in enumerate((t0, t1, t2, t3)):

        @pl.loop(0, got.shape[0])
        def _(s):
            y = (my_y - s) & 3
            for b in range(got.shape[1]):
                x = (my_x - b % 4) & 3
                c = my_c if b < 4 else 1 - my_c
                settle(pieces, got.at[s, b], ((y * 4 + x) * 2 + c) * 4 + turn)

    lay_out(pieces, out)


def rows_of(body, *got):
    _, piece = got[0].shape[-2:]
    total = sum(g.size for g in got) // piece
    return call(
        body,
        (1,),
        [whole(g.shape) for g in got],
        whole((total // PARTS, piece * PARTS)),
        jax.ShapeDtypeStruct((total // PARTS, piece * PARTS), BF16),
        (400 * total * piece, 4 * total * piece),
        [pltpu.VMEM((piece // LANES, total, LANES), F32)],
    )(*got)


def pack_body(along, rows, out, pieces):
    piece = rows.shape[1] // PARTS
    size = out.shape[1]
    here = lax.axis_index(along)
    for q in range(PARTS):
        spread(pieces, q, rows[:, q * piece : (q + 1) * piece].astype(F32))

    @pl.loop(0, out.shape[0] // 4)
    def _(d):
        for s in range(4):
            back = (here - s) & 3
            if along == "y":
                pos = back * 32 + d
            else:
                pos = (d >> 3) * 32 + back * 8 + (d & 7)
            start = pl.multiple_of((d * 4 + s) * size, 8)
            for k in range(pieces.shape[0]):
                out[pos, :, k * LANES : (k + 1) * LANES] = pieces[
                    k, pl.ds(start, size), :
                ].astype(BF16)


def pack(along, capacity, rows):
    total, width = rows.shape
    piece = width // PARTS
    shape = (total // capacity, capacity * PARTS, piece)
    return call(
        functools.partial(pack_body, along),
        (1,),
        [whole((total, width))],
        whole(shape),
        jax.ShapeDtypeStruct(shape, BF16),
        (400 * total * width, 4 * total * width),
        [pltpu.VMEM((piece // LANES, total * PARTS, LANES), F32)],
    )(rows).reshape(total * PARTS, piece)


def combine_body(weighted, key, wgt, got, out, total, pieces):
    top, tok = key.shape
    step = pl.program_id(0)
    rows = got.shape[0] // PARTS
    piece = got.shape[1]
    mine = step * rows + lax.broadcasted_iota(jnp.int32, (rows, tok), 0)
    load = jnp.zeros((rows, tok), F32)
    for j in range(top):
        load = jnp.where(mine == key[j : j + 1, :], wgt[j : j + 1, :] if weighted else 1.0, load)
    high = load.astype(BF16)
    low = (load - high.astype(F32)).astype(BF16)
    fill(pieces, got)

    @pl.when(step == 0)
    def _():
        total[...] = jnp.zeros_like(total)

    for q in range(PARTS):
        lanes = slice(q * piece, (q + 1) * piece)
        part = collected(pieces, q, 0, piece)
        more = lax.dot_general(high, part, ROWS_BY_ROWS, preferred_element_type=F32)
        if weighted:
            more = more + lax.dot_general(low, part, ROWS_BY_ROWS, preferred_element_type=F32)
        total[:, lanes] += more

    @pl.when(step == pl.num_programs(0) - 1)
    def _():
        out[...] = total[...].astype(BF16)


def combine(key, wgt, got, weighted):
    top, tok = key.shape
    count, piece = got.shape
    steps = 2
    rows = count // steps
    return call(
        functools.partial(combine_body, weighted),
        (steps,),
        [whole((top, tok))] * 2 + [pl.BlockSpec((rows, piece), lambda i: (i, 0))],
        whole((tok, piece * PARTS)),
        jax.ShapeDtypeStruct((tok, piece * PARTS), BF16),
        (4 * count * tok * piece, 2 * count * piece),
        [pltpu.VMEM((tok, piece * PARTS), F32), pltpu.VMEM((piece // LANES, rows, LANES), F32)],
    )(key, wgt, got)


def exchange(x, axes=FINE):
    return lax.all_to_all(x, axes, split_axis=0, concat_axis=0, tiled=True)


def turned(x, axis, turn):
    return lax.ppermute(x, axis, [(i, (i + turn) % 4) for i in range(4)])


def gathered(x, axis):
    return [x] + [turned(x, axis, turn) for turn in (1, 3, 2)]


def in_order(parts):
    return [parts[0], parts[1], parts[3], parts[2]]


def expert_forward(x, w_in, w_down):
    width = w_down.shape[0]
    projected = jnp.dot(x, w_in, preferred_element_type=F32)
    g, u = projected[:, :width], projected[:, width:]
    hidden = (g * jax.nn.sigmoid(g) * u).astype(BF16)
    return jnp.dot(hidden, w_down, preferred_element_type=F32).astype(BF16)


def expert_backward(projected, cot, w_in, w_down):
    width = w_down.shape[0]
    g, u = projected[:, :width], projected[:, width:]
    s = jax.nn.sigmoid(g)
    hidden = (g * s * u).astype(BF16)
    d_hidden = lax.dot_general(cot, w_down, COLS_BY_COLS, preferred_element_type=F32)
    d_gate = d_hidden * u * s * (1.0 + g * (1.0 - s))
    d_up = d_hidden * g * s
    d_proj = jnp.concatenate([d_gate, d_up], axis=1).astype(BF16)
    row_grad = lax.dot_general(
        d_proj, w_in, COLS_BY_COLS, preferred_element_type=F32
    ).astype(BF16)
    return row_grad, hidden, d_proj


def layer(
    tokens_fwd, experts_fwd, scores_fwd, tokens_bwd, experts_bwd, scores_bwd, cotangent, w_in, w_down
):
    devices = lax.axis_size(FINE)
    tok, top = experts_fwd.shape
    capacity = max(2, 3 * tok * top // (2 * devices))
    w_in, w_down = w_in[0], w_down[0]

    pay_f, key_f, wgt_f = payload(
        devices, capacity, experts_fwd.T, scores_fwd.T, (tokens_fwd,)
    )
    near_f = in_order(gathered(pay_f, "y"))
    pay_b, pay_c, key_b, wgt_b = payload(
        devices, capacity, experts_bwd.T, scores_bwd.T, (tokens_bwd, cotangent)
    )
    near_c = in_order(gathered(pay_c, "x"))
    near_b = in_order(gathered(pay_b, "z"))

    out_f = plane("y", capacity, near_f)
    in_f = exchange(out_f, ("z", "x", "c"))

    own_c = jnp.stack(near_c)
    other_c = lax.ppermute(own_c, "c", [(0, 1), (1, 0)])
    out_c = rings(capacity, own_c, other_c)
    by_y = [out_c[0]] + [turned(out_c[s], "y", s) for s in (1, 2, 3)]
    out_b = plane("z", capacity, near_b)
    out_b, in_f = lax.optimization_barrier((out_b, in_f))
    in_b = exchange(out_b, ("y", "x", "c"))

    by_z = regroup(by_y)
    in_c = [by_z[0]] + [turned(by_z[turn], "z", turn) for turn in (1, 2, 3)]
    out_rows = expert_forward(in_f, w_in, w_down)
    back_f = pack("y", capacity, out_rows)
    back_f, in_b = lax.optimization_barrier((back_f, in_b))
    home_f = exchange(back_f)

    rows_b = in_b
    projected = jnp.dot(rows_b, w_in, preferred_element_type=F32)
    cot_b = rows_of(unrings_body, *in_c)
    row_grad, hidden, d_proj = expert_backward(projected, cot_b, w_in, w_down)
    back_b = pack("z", capacity, row_grad)
    back_b, home_f = lax.optimization_barrier((back_b, home_f))
    home_b = exchange(back_b)

    output_fwd = combine(key_f, wgt_f, home_f, True)
    grad_down = lax.dot_general(
        hidden, cot_b, ROWS_BY_ROWS, preferred_element_type=F32
    ).astype(BF16)
    grad_in = lax.dot_general(
        rows_b, d_proj, ROWS_BY_ROWS, preferred_element_type=F32
    ).astype(BF16)
    grad_tokens = combine(key_b, wgt_b, home_b, False)
    return output_fwd, grad_tokens, grad_in[None], grad_down[None]


def solution(mesh):
    rows = P(FINE, None)
    cube = P(FINE, None, None)
    fine = Mesh(mesh.devices.reshape(4, 4, 4, 2), FINE)
    return jax.shard_map(
        layer,
        mesh=fine,
        in_specs=(rows,) * 7 + (cube,) * 2,
        out_specs=(rows, rows, cube, cube),
        check_vma=False,
    )
```
